256 devices in a mesh: gx: 16 (over z, x_lo), gy: 8 (over y, x_hi), gz: 2 (over core).
Axes of the slice: x: 4 (x_hi: 2, x_lo: 2; x = x_hi * 2 + x_lo), y: 4, z: 8, core: 2. Of those that a mesh axis runs over, the one named last changes fastest.
Arguments:
- patches: bfloat16 [16, 8, 3, 64, 64, 256], P(None, 'gy', None, 'gx', None, 'gz'), may hold values from -8 to 308
Outputs:
- smooth: float32 [3, 512, 256, 128], P(None, 'gx', 'gy', 'gz')
- confidence: float32 [512, 256, 128], P('gx', 'gy', 'gz')
The draws below stay inside these ranges and needn't reach their ends.
All inputs are finite; a program needn't handle non-finite values.
Results may differ from the reference program's by a relative error of at most 0.0013.
Values may be sent and summed in bfloat16 or wider, within the bound.
A program may use at most 192 MiB of HBM per device.

```python
import jax
import jax.numpy as jnp
from jax import lax

P_SIZE = 64
C = 3
NPX = 16
NPY = 8
NPZ = 4


def draw_patches(key, part):
    dims_all = (NPX, NPY, C, P_SIZE, P_SIZE, NPZ, P_SIZE)
    first_key = jax.random.fold_in(jax.random.fold_in(key, 17), 0)
    values = jnp.clip(2.0 * jax.random.normal(first_key, dims_all, jnp.float32), -8.0, 8.0)
    return values.reshape(NPX, NPY, C, P_SIZE, P_SIZE, NPZ * P_SIZE).astype(jnp.bfloat16)


def setup_inputs(seed: int = 0) -> dict:
    key_list = jax.random.split(jax.random.key(seed), 2)
    return {
        "patches": draw_patches(jax.random.fold_in(key_list[1], 71), 0),
    }


def gaussian(offsets, length):
    centre = (length - 1) / 2.0
    spread = length / 8.0
    return jnp.exp(-(offsets - centre) ** 2 / (2.0 * spread * spread))


def place_halves(values, axis_k, axis_h):
    leading = lax.index_in_dim(values, 0, axis_h, keepdims=False)
    trailing = lax.index_in_dim(values, 1, axis_h, keepdims=False)
    step = leading.shape[axis_k] // max(leading.shape[axis_k], 1)
    lead_pad = [(0, 0)] * leading.ndim
    trail_pad = [(0, 0)] * leading.ndim
    lead_pad[axis_k] = (0, 1)
    trail_pad[axis_k] = (1, 0)
    return jnp.pad(leading, lead_pad) + jnp.pad(trailing, trail_pad) * step


def fold_inner(weighted, stride):
    count_a, count_b, classes, length, _, depth = weighted.shape
    count_c = depth // length
    folded = weighted.reshape(count_a, count_b, classes, length, length, count_c, 2, stride)
    folded = place_halves(folded, 5, 6)
    depth_cells = (count_c + 1) * stride
    folded = folded.reshape(count_a, count_b, classes, length, 2, stride, depth_cells)
    folded = place_halves(folded, 1, 4)
    wide_cells = (count_b + 1) * stride
    folded = folded.transpose(0, 2, 3, 1, 4, 5)
    return folded.reshape(count_a, classes, 2, stride, wide_cells, depth_cells)


def fold_outer(folded):
    count_a, classes, _, stride, wide_cells, depth_cells = folded.shape
    placed = place_halves(folded, 0, 2)
    return placed.transpose(1, 0, 2, 3, 4).reshape(classes, (count_a + 1) * stride, wide_cells, depth_cells)


def weight_line(begin_at, number, stride):
    cells = begin_at + jnp.arange(number, dtype=jnp.int32)
    cell_index = cells // stride
    near_offset = (cells - cell_index * stride).astype(jnp.float32)
    length = 2 * stride
    line = gaussian(near_offset, length)
    return line + jnp.where(cell_index >= 1, gaussian(near_offset + stride, length), 0.0)


def count_line(begin_at, number, extent):
    cells = begin_at + jnp.arange(number, dtype=jnp.int32)
    return 3.0 - (cells == 0).astype(jnp.float32) - (cells == extent - 1).astype(jnp.float32)


def box_sum(padded):
    summed = padded[:, :, :, :-2] + padded[:, :, :, 1:-1] + padded[:, :, :, 2:]
    summed = summed[:, :, :-2] + summed[:, :, 1:-1] + summed[:, :, 2:]
    return summed[:, :-2] + summed[:, 1:-1] + summed[:, 2:]


def reference(patches):
    pos_x, pos_y, classes, length, _, depth = patches.shape
    stride = length // 2
    pos_z = depth // length
    profile = gaussian(jnp.arange(length).astype(jnp.float32), length)
    factor = profile[:, None, None] * profile[None, :, None] * jnp.tile(profile, pos_z)[None, None, :]

    def one_row(row):
        weighted = row[None].astype(jnp.float32) * factor
        return fold_inner(weighted, stride)[0]

    rows = lax.map(one_row, patches)
    accumulated = fold_outer(rows)
    cells_x, cells_y, cells_z = pos_x * stride, pos_y * stride, pos_z * stride
    accumulated = accumulated[:, :cells_x, :cells_y, :cells_z]
    line_x = weight_line(0, cells_x, stride)
    line_y = weight_line(0, cells_y, stride)
    line_z = weight_line(0, cells_z, stride)
    weight_sum = line_x[:, None, None] * line_y[None, :, None] * line_z[None, None, :]
    logits = accumulated / weight_sum
    probability = jax.nn.softmax(logits, axis=0)
    padded = jnp.pad(probability, ((0, 0), (1, 1), (1, 1), (1, 1)))
    counts = count_line(0, cells_x, cells_x)[:, None, None] * count_line(0, cells_y, cells_y)[None, :, None]
    counts = counts * count_line(0, cells_z, cells_z)[None, None, :]
    smooth = box_sum(padded) / counts
    return smooth, jnp.max(smooth, axis=0)
```

```python
import functools

import jax
import jax.numpy as jnp
from jax import lax
from jax.experimental import pallas as pl
from jax.experimental.pallas import tpu as pltpu
from jax.sharding import PartitionSpec as P

MESH = pl.DeviceIdType.MESH
F32 = jnp.float32
WIRE = jnp.float32


def gauss(offset):
    return jnp.exp(-((offset - 31.5) ** 2) / 128.0)


def filled(scalar, shape):
    return jnp.full(shape, scalar, F32)


def kernel(
    patches,
    smooth,
    conf,
    raw,
    part,
    weight,
    own,
    up_same,
    low_cross,
    up_cross,
    got_up_same,
    got_low_cross,
    got_up_cross,
    folded,
    slots,
    prob,
    column,
    got_column,
    rows,
    got_rows,
    summed,
    got_planes,
    load_sem,
    part_sem,
    x_send,
    x_recv,
    z_send,
    z_recv,
    h_send,
    h_recv,
):
    gx, gy, gz = lax.axis_index("gx"), lax.axis_index("gy"), lax.axis_index("gz")
    zc, xl = gx // 2, lax.rem(gx, 2)
    half = zc // 4
    xo = 1 - xl
    y_up, y_down = lax.rem(gy + 1, 8), lax.rem(gy + 7, 8)
    gx_up, gx_down = lax.rem(gx + 1, 16), lax.rem(gx + 15, 16)
    gx_cross = zc * 2 + xo
    partner = (gx, gy, 1 - gz)
    first = gz == 1

    def offset(k):
        odd = lax.rem(k, 2)
        return odd * ((9 + k) // 2) + (1 - odd) * ((8 - k) // 2)

    def target(k):
        return lax.rem(zc + offset(k), 8)

    def patch_of(k, side):
        a = 2 * target(k) + (xl if side == 0 else xo) - half
        return jnp.maximum(a, 0), (a >= 0).astype(F32)

    def load(k, side):
        a, _ = patch_of(k, side)
        return pltpu.make_async_copy(
            patches.at[a, 0], raw.at[2 * k + side], load_sem.at[2 * k + side]
        )

    def start_loads(k, _):
        load(k, 0).start()
        load(k, 1).start()
        return 0

    lax.fori_loop(0, 8, start_loads, 0)

    peers = [
        partner,
        (gx, y_up, gz),
        (gx, y_down, gz),
        (gx_cross, gy, gz),
        (gx_cross, y_up, gz),
        (gx_cross, y_down, gz),
        (lax.rem(gx + 15 + 2 * xl, 16), gy, gz),
    ]
    for d in range(1, 8):
        peers.append((lax.rem(gx + 2 * d, 16), gy, gz))
    barrier = pltpu.get_barrier_semaphore()
    for peer in peers:
        pl.semaphore_signal(barrier, inc=1, device_id=peer, device_id_type=MESH)

    lane = lax.broadcasted_iota(jnp.int32, (64, 128), 1)
    cell = lax.broadcasted_iota(jnp.int32, (64, 128), 0)
    plane = gauss(cell.astype(F32)) * gauss(lax.rem(lane, 64).astype(F32))
    sent_up = (gy < 7).astype(F32)
    plane = jnp.where(cell >= 32, plane * sent_up, plane)
    for u in range(4):
        row = (4 * gx + u).astype(F32)
        weight[u] = plane * gauss(filled(row, (64, 128)))

    pl.semaphore_wait(barrier, len(peers))

    def send_part(k, side):
        a, _ = patch_of(k, side)
        return pltpu.make_async_remote_copy(
            src_ref=patches.at[a, 0],
            dst_ref=part.at[2 * k + side],
            send_sem=part_sem.at[0, 2 * k + side],
            recv_sem=part_sem.at[1, 2 * k + side],
            device_id=partner,
            device_id_type=MESH,
        )

    @pl.when(gz == 0)
    def _():
        def start(k, _):
            send_part(k, 0).start()
            send_part(k, 1).start()
            return 0

        lax.fori_loop(0, 8, start, 0)

    quarter = lane // 32
    wrap_gain = jnp.where(
        (quarter == 0) | (quarter == 2), filled(first.astype(F32), (64, 128)), 1.0
    )
    last_quarter = lane >= 96
    from_part = last_quarter & (filled(first.astype(F32), (64, 128)) > 0.5)
    low_half = lane < 64
    outer = (quarter == 0) | (quarter == 3)

    def x_copies(k):
        t = target(k)
        plan = (
            (up_same, got_up_same, (gx, y_up, gz)),
            (low_cross, got_low_cross, (gx_cross, gy, gz)),
            (up_cross, got_up_cross, (gx_cross, y_up, gz)),
        )
        return [
            pltpu.make_async_remote_copy(
                src_ref=src.at[t],
                dst_ref=dst.at[t],
                send_sem=x_send.at[i, t],
                recv_sem=x_recv.at[i, t],
                device_id=device,
                device_id_type=MESH,
            )
            for i, (src, dst, device) in enumerate(plan)
        ]

    def fold(k, _):
        t = target(k)
        for side in (1, 0):
            load(k, side).wait()

            @pl.when(gz == 1)
            def _():
                send_part(k, side).wait_recv()

            _, valid = patch_of(k, side)
            for u in range(4):
                w = weight[u] * valid
                p = []
                for c in range(3):
                    mine = raw[2 * k + side, c, u].astype(F32)
                    theirs = part[2 * k + side, c, u].astype(F32)
                    p.append(jnp.where(from_part, theirs, mine))
                x1 = (p[1] - p[0]) * w
                x2 = (p[2] - p[0]) * w
                base = jnp.where(low_half, x1, pltpu.roll(x2, 64, 1))
                a1 = pltpu.roll(jnp.where(last_quarter, x1, x2), 32, 1)
                a2 = pltpu.roll(jnp.where(last_quarter, x2, x1), 96, 1)
                d = base + jnp.where(outer, a1, a2) * wrap_gain
                if side == 0:
                    own[t, u] = d[:32]
                    up_same[t, u] = d[32:]
                else:
                    low_cross[t, u] = d[:32]
                    up_cross[t, u] = d[32:]
        for copy in x_copies(k):
            copy.start()
        return 0

    lax.fori_loop(0, 8, fold, 0)

    def z_copy(k):
        t = target(k)
        return pltpu.make_async_remote_copy(
            src_ref=folded.at[t],
            dst_ref=slots.at[zc],
            send_sem=z_send.at[t],
            recv_sem=z_recv.at[zc],
            device_id=(2 * t + xl, gy, gz),
            device_id_type=MESH,
        )

    def forward(k, dst):
        t = target(k)
        for copy in x_copies(k):
            copy.wait_recv()
        place = t if dst is folded else zc
        dst[place, pl.ds(4 * xl, 4)] = own[t] + got_up_same[t]
        dst[place, pl.ds(4 * xo, 4)] = got_low_cross[t] + got_up_cross[t]

    def pass_on(k, _):
        forward(k, folded)
        z_copy(k).start()
        return 0

    lax.fori_loop(0, 7, pass_on, 0)
    forward(jnp.int32(7), slots)

    lane = lax.broadcasted_iota(jnp.int32, (32, 128), 1)
    cell = lax.broadcasted_iota(jnp.int32, (32, 128), 0)

    def line(offsets, later):
        return gauss(offsets) + later * gauss(offsets + 32.0)

    line_y = line(cell.astype(F32), (gy >= 1).astype(F32))
    z_later = jnp.where(lax.rem(lane, 64) >= 32, 1.0, filled(first.astype(F32), (32, 128)))
    line_z = line(lax.rem(lane, 32).astype(F32), z_later)
    x_later = (gx >= 1).astype(F32)

    def await_slot(s):
        @pl.when(zc != s)
        def _():
            pltpu.make_async_remote_copy(
                src_ref=folded.at[0],
                dst_ref=slots.at[s],
                send_sem=z_send.at[0],
                recv_sem=z_recv.at[s],
                device_id=(gx, gy, 1 - gz),
                device_id_type=MESH,
            ).wait_recv()

    def softmax(s, _):
        await_slot(s)
        await_slot(s + 4)
        for i in range(8):
            x = 8 * s + i
            total = slots[s, i] + slots[s + 4, i]
            line_x = line(filled(x.astype(F32), (32, 128)), x_later)
            d = total / (line_x * line_y * line_z)
            top = jnp.maximum(jnp.maximum(d, pltpu.roll(d, 64, 1)), 0.0)
            e = jnp.exp(d - top)
            prob[x] = e / (e + pltpu.roll(e, 64, 1) + jnp.exp(-top))
        return 0

    lax.fori_loop(0, 4, softmax, 0)

    is_first = filled(first.astype(F32), (32, 128))
    in_lane = lax.rem(lane, 64)
    shift_out = 65 * (1 - gz)
    shift_in = 63 + 65 * gz

    def pack(x, packed):
        moved = pltpu.roll(prob[x], x + shift_out, 1)
        return jnp.where(in_lane == x, moved, packed)

    column[...] = lax.fori_loop(0, 32, pack, jnp.zeros((32, 128), F32))

    def exchange(i, src, dst, device):
        return pltpu.make_async_remote_copy(
            src_ref=src,
            dst_ref=dst,
            send_sem=h_send.at[i],
            recv_sem=h_recv.at[i],
            device_id=device,
            device_id_type=MESH,
        )

    z_halo = exchange(0, column, got_column, partner)
    z_halo.start()
    z_halo.wait()

    def sum_z(x, _):
        p = prob[x]
        edge = pltpu.roll(got_column[...], lax.rem(shift_in - x, 128), 1)
        before = jnp.where(in_lane == 0, edge * is_first, pltpu.roll(p, 1, 1))
        after = jnp.where(in_lane == 63, edge * (1.0 - is_first), pltpu.roll(p, 127, 1))
        total = before + p + after
        prob[x] = total
        rows[0, pl.ds(x, 1)] = total[0:1]
        rows[1, pl.ds(x, 1)] = total[31:32]
        return 0

    lax.fori_loop(0, 32, sum_z, 0)
    y_halo = [
        exchange(1, rows.at[0], got_rows.at[1], (gx, y_down, gz)),
        exchange(2, rows.at[1], got_rows.at[0], (gx, y_up, gz)),
    ]
    for copy in y_halo:
        copy.start()
    for copy in y_halo:
        copy.wait()
    y_before, y_after = (gy > 0).astype(F32), (gy < 7).astype(F32)

    def sum_y(x, _):
        s = prob[x]
        low = jnp.broadcast_to(got_rows[0, pl.ds(x, 1)] * y_before, (32, 128))
        high = jnp.broadcast_to(got_rows[1, pl.ds(x, 1)] * y_after, (32, 128))
        before = jnp.where(cell == 0, low, pltpu.roll(s, 1, 0))
        after = jnp.where(cell == 31, high, pltpu.roll(s, 31, 0))
        summed[x + 1] = before + s + after
        return 0

    lax.fori_loop(0, 32, sum_y, 0)
    x_halo = [
        exchange(3, summed.at[1], got_planes.at[1], (gx_down, gy, gz)),
        exchange(4, summed.at[32], got_planes.at[0], (gx_up, gy, gz)),
    ]
    for copy in x_halo:
        copy.start()
    for copy in x_halo:
        copy.wait()
    summed[0] = got_planes[0] * (gx > 0).astype(F32)
    summed[33] = got_planes[1] * (gx < 15).astype(F32)

    count_y = (
        3.0
        - jnp.where(cell == 0, 1.0 - y_before, 0.0)
        - jnp.where(cell == 31, 1.0 - y_after, 0.0)
    )
    count_z = (
        3.0
        - jnp.where(in_lane == 0, 1.0 - is_first, 0.0)
        - jnp.where(in_lane == 63, is_first, 0.0)
    )
    inverse = 1.0 / (count_y * count_z)

    def sum_x(x, _):
        total = summed[x] + summed[x + 1] + summed[x + 2]
        cut = ((gx == 0) & (x == 0)) | ((gx == 15) & (x == 31))
        count_x = 3.0 - filled(cut.astype(F32), (32, 128))
        s1 = total * (inverse / count_x)
        s2 = pltpu.roll(s1, 64, 1)
        s0 = 1.0 - s1 - s2
        smooth[0, x] = s0[:, :64]
        smooth[1, x] = s1[:, :64]
        smooth[2, x] = s2[:, :64]
        conf[x] = jnp.maximum(jnp.maximum(s0, s1), s2)[:, :64]
        return 0

    lax.fori_loop(0, 32, sum_x, 0)

    @pl.when(gz == 0)
    def _():
        def finish(k, _):
            send_part(k, 0).wait_send()
            send_part(k, 1).wait_send()
            return 0

        lax.fori_loop(0, 8, finish, 0)

    def finish(k, _):
        for copy in x_copies(k):
            copy.wait_send()
        return 0

    lax.fori_loop(0, 8, finish, 0)

    def finish_z(k, _):
        z_copy(k).wait_send()
        return 0

    lax.fori_loop(0, 7, finish_z, 0)


def per_device(patches):
    vmem = pltpu.VMEM
    dma = pltpu.SemaphoreType.DMA
    any_space = pl.BlockSpec(memory_space=pl.ANY)
    in_vmem = pl.BlockSpec(memory_space=pltpu.VMEM)
    return pl.pallas_call(
        kernel,
        name="stitch",
        out_shape=(
            jax.ShapeDtypeStruct((3, 32, 32, 64), F32),
            jax.ShapeDtypeStruct((32, 32, 64), F32),
        ),
        in_specs=[any_space],
        out_specs=(in_vmem, in_vmem),
        scratch_shapes=[
            vmem((16, 3, 4, 64, 128), jnp.bfloat16),
            vmem((16, 3, 4, 64, 128), jnp.bfloat16),
            vmem((4, 64, 128), F32),
            vmem((8, 4, 32, 128), F32),
            *[vmem((8, 4, 32, 128), WIRE)] * 6,
            vmem((8, 8, 32, 128), WIRE),
            vmem((8, 8, 32, 128), WIRE),
            vmem((32, 32, 128), F32),
            vmem((32, 128), F32),
            vmem((32, 128), F32),
            vmem((2, 32, 128), F32),
            vmem((2, 32, 128), F32),
            vmem((34, 32, 128), F32),
            vmem((2, 32, 128), F32),
            dma((16,)),
            dma((2, 16)),
            dma((3, 8)),
            dma((3, 8)),
            dma((8,)),
            dma((8,)),
            dma((5,)),
            dma((5,)),
        ],
        compiler_params=pltpu.CompilerParams(
            collective_id=0, has_side_effects=True, vmem_limit_bytes=60 << 20
        ),
    )(patches)


def solution(mesh):
    in_specs = (P(None, "gy", None, "gx", None, "gz"),)
    out_specs = (P(None, "gx", "gy", "gz"), P("gx", "gy", "gz"))
    return jax.shard_map(
        per_device, mesh=mesh, in_specs=in_specs, out_specs=out_specs, check_vma=False
    )
```

```python
import jax
import jax.numpy as jnp
from jax import lax
from jax.experimental import pallas as pl
from jax.experimental.pallas import tpu as pltpu
from jax.sharding import PartitionSpec as P

MESH = pl.DeviceIdType.MESH
F32 = jnp.float32
WIRE = jnp.bfloat16

BASE = 125.5
GAIN = 252.7 / 316.0
SPREAD = 0.05


def gauss(offset):
    return jnp.exp(-((offset - 31.5) ** 2) / 128.0)


def filled(scalar, shape):
    return jnp.full(shape, scalar, F32)


def encode(value, dither):
    size = jnp.exp2(jnp.abs(value) * GAIN + dither)
    return jnp.where(value < 0, -size, size).astype(WIRE)


def decode(code, dither):
    code = code.astype(F32)
    size = jnp.log2(jnp.abs(code)) * (1.0 / GAIN) - dither * (1.0 / GAIN)
    return jnp.where(code < 0, -size, size)


def share(offset):
    near = gauss(offset)
    return near / (near + gauss(offset + 32.0))


def kernel(
    patches,
    sums,
    side_sums,
    raw,
    part,
    own,
    up_same,
    low_cross,
    up_cross,
    got_up_same,
    got_low_cross,
    got_up_cross,
    folded,
    slots,
    dither,
    prob,
    got_block,
    rows,
    corners,
    got_planes,
    got_rows,
    got_corners,
    load_sem,
    part_sem,
    x_send,
    x_recv,
    z_send,
    z_recv,
    h_send,
    h_recv,
):
    gx, gy, gz = lax.axis_index("gx"), lax.axis_index("gy"), lax.axis_index("gz")
    zc, xl = gx // 2, lax.rem(gx, 2)
    half = zc // 4
    xo = 1 - xl
    gx_by = {1: lax.rem(gx + 1, 16), 0: gx, -1: lax.rem(gx + 15, 16)}
    gy_by = {1: lax.rem(gy + 1, 8), 0: gy, -1: lax.rem(gy + 7, 8)}
    gx_cross = zc * 2 + xo
    partner = (gx, gy, 1 - gz)

    def target(k):
        odd = lax.rem(k, 2)
        return lax.rem(zc + odd * ((9 + k) // 2) + (1 - odd) * ((8 - k) // 2), 8)

    def load(k, side):
        a = jnp.maximum(2 * target(k) + (xl if side == 0 else xo) - half, 0)
        return pltpu.make_async_copy(
            patches.at[a, 0], raw.at[2 * k + side], load_sem.at[2 * k + side]
        )

    def start_loads(k, _):
        load(k, 1).start()
        load(k, 0).start()
        return 0

    lax.fori_loop(0, 8, start_loads, 0)

    around = [(i, j) for i in (-1, 0, 1) for j in (-1, 0, 1) if i or j]
    peers = [partner]
    for i, j in around:
        peers.append((gx_by[i], gy_by[j], gz))
        peers.append((gx_by[i], gy_by[j], 1 - gz))
    for d in range(1, 8):
        peers.append((lax.rem(gx + 2 * d, 16), gy, gz))
    barrier = pltpu.get_barrier_semaphore()
    for peer in peers:
        pl.semaphore_signal(barrier, inc=1, device_id=peer, device_id_type=MESH)

    lane = lax.broadcasted_iota(jnp.int32, (64, 128), 1)
    core = filled(gz.astype(F32), (64, 128))
    offset = lax.rem(lane, 64).astype(F32)
    inner = lax.rem(lane, 32).astype(F32)
    weight = gauss(offset) / (gauss(inner) + gauss(inner + 32.0))
    weight = jnp.where(lane < 32, jnp.where(core > 0.5, weight, 1.0), weight)
    last_quarter = lane >= 96
    weight = jnp.where(last_quarter, weight * core, weight)
    from_part = last_quarter & (core > 0.5)
    low_half = lane < 64
    outer = (lane < 32) | last_quarter

    number = lax.broadcasted_iota(jnp.int32, (32, 128), 0) * 128 + lax.broadcasted_iota(
        jnp.int32, (32, 128), 1
    )
    for u in range(8):
        mixed = (number + 4096 * u + 1) * 40503
        mixed = (mixed + mixed // 512) * 30269
        bits = (mixed // 256) & 1023
        dither[u] = bits.astype(F32) * (SPREAD / 1024.0) - BASE

    def send_part(k, side):
        return pltpu.make_async_remote_copy(
            src_ref=raw.at[2 * k + side],
            dst_ref=part.at[2 * k + side],
            send_sem=part_sem.at[0, 2 * k + side],
            recv_sem=part_sem.at[1, 2 * k + side],
            device_id=partner,
            device_id_type=MESH,
        )

    def x_copies(k):
        t = target(k)
        plan = (
            (low_cross, got_low_cross, (gx_cross, gy, gz)),
            (up_cross, got_up_cross, (gx_cross, gy_by[1], gz)),
            (up_same, got_up_same, (gx, gy_by[1], gz)),
        )
        return [
            pltpu.make_async_remote_copy(
                src_ref=src.at[t],
                dst_ref=dst.at[t],
                send_sem=x_send.at[i, t],
                recv_sem=x_recv.at[i, t],
                device_id=device,
                device_id_type=MESH,
            )
            for i, (src, dst, device) in enumerate(plan)
        ]

    def fold(k, side):
        t = target(k)
        for u in range(4):
            p = []
            for c in range(3):
                mine = raw[2 * k + side, c, u].astype(F32)
                theirs = part[2 * k + side, c, u].astype(F32)
                p.append(jnp.where(from_part, theirs, mine))
            x1 = (p[1] - p[0]) * weight
            x2 = (p[2] - p[0]) * weight
            base = jnp.where(low_half, x1, pltpu.roll(x2, 64, 1))
            a1 = pltpu.roll(jnp.where(last_quarter, x1, x2), 32, 1)
            a2 = pltpu.roll(jnp.where(last_quarter, x2, x1), 96, 1)
            d = base + jnp.where(outer, a1, a2)
            if side == 0:
                own[t, u] = d[:32]
                up_same[t, u] = encode(d[32:], dither[u])
            else:
                low_cross[t, u] = encode(d[:32], dither[u])
                up_cross[t, u] = encode(d[32:], dither[u])

    def fold_early(k, _):
        for side in (1, 0):
            load(k, side).wait()
            fold(k, side)
        return 0

    lax.fori_loop(0, 8 * (1 - gz), fold_early, 0)
    pl.semaphore_wait(barrier, len(peers))

    @pl.when(gz == 0)
    def _():
        def start_part(k, _):
            send_part(k, 1).start()
            send_part(k, 0).start()
            return 0

        lax.fori_loop(0, 8, start_part, 0)

        def start_x(k, _):
            for copy in x_copies(k):
                copy.start()
            return 0

        lax.fori_loop(0, 8, start_x, 0)

    def fold_late(k, _):
        for side in (1, 0):
            load(k, side).wait()
            send_part(k, side).wait_recv()
            fold(k, side)
        for copy in x_copies(k):
            copy.start()
        return 0

    lax.fori_loop(0, 8 * gz, fold_late, 0)

    cell = lax.broadcasted_iota(jnp.int32, (32, 128), 0)
    has_below = filled((gy >= 1).astype(F32), (32, 128))
    high_y = (1.0 - share(cell.astype(F32))) * has_below
    low_y = 1.0 - high_y

    def z_copy(k):
        t = target(k)
        return pltpu.make_async_remote_copy(
            src_ref=folded.at[t],
            dst_ref=slots.at[zc],
            send_sem=z_send.at[t],
            recv_sem=z_recv.at[zc],
            device_id=(2 * t + xl, gy, gz),
            device_id_type=MESH,
        )

    def forward(k, dst, place):
        t = target(k)
        for copy in x_copies(k):
            copy.wait_recv()
        for u in range(4):
            same = low_y * own[t, u] + high_y * decode(got_up_same[t, u], dither[u])
            cross = low_y * decode(got_low_cross[t, u], dither[u])
            cross += high_y * decode(got_up_cross[t, u], dither[u])
            dst[place, 4 * xl + u] = encode(same, dither[4 + u])
            dst[place, 4 * xo + u] = encode(cross, dither[4 + u])

    def pass_on(k, _):
        forward(k, folded, target(k))
        z_copy(k).start()
        return 0

    lax.fori_loop(0, 7, pass_on, 0)
    forward(jnp.int32(7), slots, zc)

    def await_slot(s):
        @pl.when(zc != s)
        def _():
            pltpu.make_async_remote_copy(
                src_ref=folded.at[0],
                dst_ref=slots.at[s],
                send_sem=z_send.at[0],
                recv_sem=z_recv.at[s],
                device_id=partner,
                device_id_type=MESH,
            ).wait_recv()

    has_before = (gx >= 1).astype(F32)

    def softmax(s, _):
        await_slot(s)
        await_slot(s + 4)
        for i in range(8):
            x = 8 * s + i
            high_x = (1.0 - share(filled(x.astype(F32), (1, 128)))) * has_before
            near = decode(slots[s, i], dither[4 + i % 4])
            far = decode(slots[s + 4, i], dither[4 + i % 4])
            d = near + high_x * (far - near)
            top = jnp.maximum(jnp.maximum(d, pltpu.roll(d, 64, 1)), 0.0)
            e = jnp.exp(d - top)
            p = e / (e + pltpu.roll(e, 64, 1) + jnp.exp(-top))
            prob[x] = p
            rows[0, pl.ds(x, 1)] = p[0:1]
            rows[1, pl.ds(x, 1)] = p[31:32]
        return 0

    lax.fori_loop(0, 4, softmax, 0)
    for i in range(2):
        for j in range(2):
            corners[2 * i + j] = rows[j, 31 * i : 31 * i + 1]

    halos = []

    def exchange(src, dst, device):
        n = len(halos)
        halos.append(
            pltpu.make_async_remote_copy(
                src_ref=src,
                dst_ref=dst,
                send_sem=h_send.at[n],
                recv_sem=h_recv.at[n],
                device_id=device,
                device_id_type=MESH,
            )
        )
        halos[-1].start()

    for other in range(2):
        to = 1 - gz if other else gz
        for i in range(2):
            for j in range(2):
                exchange(
                    corners.at[2 * i + j],
                    got_corners.at[other, 2 * (1 - i) + 1 - j],
                    (gx_by[2 * i - 1], gy_by[2 * j - 1], to),
                )
    for other in range(2):
        to = 1 - gz if other else gz
        for i in range(2):
            exchange(rows.at[i], got_rows.at[other, 1 - i], (gx, gy_by[2 * i - 1], to))
        for i in range(2):
            exchange(
                prob.at[31 * i], got_planes.at[other, 1 - i], (gx_by[2 * i - 1], gy, to)
            )
    exchange(prob, got_block, partner)

    def sum_z(p, q):
        at = lax.rem(lax.broadcasted_iota(jnp.int32, p.shape, 1), 64)
        upper = filled(gz.astype(F32), p.shape)
        edge = pltpu.roll(q, 63 + 2 * gz, 1)
        before = jnp.where(at == 0, edge * upper, pltpu.roll(p, 1, 1))
        after = jnp.where(at == 63, edge * (1.0 - upper), pltpu.roll(p, 127, 1))
        return before + p + after

    halos[-1].wait_recv()

    def sum_block(s, _):
        for i in range(4):
            sums[4 * s + i + 1] = sum_z(prob[4 * s + i], got_block[4 * s + i])
        return 0

    lax.fori_loop(0, 8, sum_block, 0)
    for copy in halos[:-1]:
        copy.wait_recv()
    inside_x = ((gx > 0).astype(F32), (gx < 15).astype(F32))
    inside_y = ((gy > 0).astype(F32), (gy < 7).astype(F32))
    for i in range(2):
        sums[33 * i] = sum_z(got_planes[0, i], got_planes[1, i]) * inside_x[i]
    for j in range(2):
        side_sums[j, 1:33] = sum_z(got_rows[0, j], got_rows[1, j]) * inside_y[j]
        for i in range(2):
            n = 2 * i + j
            corner = sum_z(
                jnp.broadcast_to(got_corners[0, n], (8, 128)),
                jnp.broadcast_to(got_corners[1, n], (8, 128)),
            )
            side_sums[j, 33 * i : 33 * i + 1] = corner[0:1] * (inside_x[i] * inside_y[j])

    @pl.when(gz == 0)
    def _():
        def finish(k, _):
            send_part(k, 0).wait_send()
            send_part(k, 1).wait_send()
            return 0

        lax.fori_loop(0, 8, finish, 0)

    def finish(k, _):
        for copy in x_copies(k):
            copy.wait_send()
        return 0

    lax.fori_loop(0, 8, finish, 0)

    def finish_z(k, _):
        z_copy(k).wait_send()
        return 0

    lax.fori_loop(0, 7, finish_z, 0)
    for copy in halos:
        copy.wait_send()


def box(sums, side_sums, smooth, conf, sides):
    gx, gy, gz = lax.axis_index("gx"), lax.axis_index("gy"), lax.axis_index("gz")
    step = pl.program_id(0)
    count = smooth.shape[1]
    lane = lax.rem(lax.broadcasted_iota(jnp.int32, (32, 128), 1), 64)
    cell = lax.broadcasted_iota(jnp.int32, (32, 128), 0)

    def cut(place, at, there):
        return jnp.where(place == at, filled(there.astype(F32), (32, 128)), 0.0)

    count_y = 3.0 - cut(cell, 0, gy == 0) - cut(cell, 31, gy == 7)
    count_z = 3.0 - cut(lane, 0, gz == 0) - cut(lane, 63, gz == 1)
    inverse = 1.0 / (count_y * count_z)
    for j in range(2):
        sides[j] = side_sums[j, 0:32] + side_sums[j, 1:33] + side_sums[j, 2:34]
    for i in range(count):
        x = step * count + i
        s = sums[x] + sums[x + 1] + sums[x + 2]
        low = jnp.broadcast_to(sides[0, pl.ds(x, 1)], (32, 128))
        high = jnp.broadcast_to(sides[1, pl.ds(x, 1)], (32, 128))
        before = jnp.where(cell == 0, low, pltpu.roll(s, 1, 0))
        after = jnp.where(cell == 31, high, pltpu.roll(s, 31, 0))
        end = ((gx == 0) & (x == 0)) | ((gx == 15) & (x == 31))
        count_x = 3.0 - filled(end.astype(F32), (32, 128))
        s1 = (before + s + after) * (inverse / count_x)
        s2 = pltpu.roll(s1, 64, 1)
        s0 = 1.0 - s1 - s2
        smooth[0, i] = s0[:, :64]
        smooth[1, i] = s1[:, :64]
        smooth[2, i] = s2[:, :64]
        conf[i] = jnp.maximum(jnp.maximum(s0, s1), s2)[:, :64]


def per_device(patches):
    vmem = pltpu.VMEM
    dma = pltpu.SemaphoreType.DMA
    in_hbm = pl.BlockSpec(memory_space=pltpu.HBM)
    in_vmem = pl.BlockSpec(memory_space=pltpu.VMEM)
    sums, side_sums = pl.pallas_call(
        kernel,
        name="stitch",
        out_shape=(
            jax.ShapeDtypeStruct((34, 32, 128), F32),
            jax.ShapeDtypeStruct((2, 40, 128), F32),
        ),
        in_specs=[in_hbm],
        out_specs=(in_vmem, in_vmem),
        scratch_shapes=[
            vmem((16, 3, 4, 64, 128), jnp.bfloat16),
            vmem((16, 3, 4, 64, 128), jnp.bfloat16),
            vmem((8, 4, 32, 128), F32),
            *[vmem((8, 4, 32, 128), WIRE)] * 6,
            vmem((8, 8, 32, 128), WIRE),
            vmem((8, 8, 32, 128), WIRE),
            vmem((8, 32, 128), F32),
            vmem((32, 32, 128), F32),
            vmem((32, 32, 128), F32),
            vmem((2, 32, 128), F32),
            vmem((4, 1, 128), F32),
            vmem((2, 2, 32, 128), F32),
            vmem((2, 2, 32, 128), F32),
            vmem((2, 4, 1, 128), F32),
            dma((16,)),
            dma((2, 16)),
            dma((3, 8)),
            dma((3, 8)),
            dma((8,)),
            dma((8,)),
            dma((17,)),
            dma((17,)),
        ],
        compiler_params=pltpu.CompilerParams(
            collective_id=0, has_side_effects=True, vmem_limit_bytes=52 << 20
        ),
    )(patches)
    steps = 4
    return pl.pallas_call(
        box,
        name="box",
        grid=(steps,),
        out_shape=(
            jax.ShapeDtypeStruct((3, 32, 32, 64), F32),
            jax.ShapeDtypeStruct((32, 32, 64), F32),
        ),
        in_specs=[in_vmem, in_vmem],
        out_specs=(
            pl.BlockSpec((3, 32 // steps, 32, 64), lambda i: (0, i, 0, 0)),
            pl.BlockSpec((32 // steps, 32, 64), lambda i: (i, 0, 0)),
        ),
        scratch_shapes=[vmem((2, 32, 128), F32)],
        compiler_params=pltpu.CompilerParams(vmem_limit_bytes=20 << 20),
    )(sums, side_sums)


def solution(mesh):
    in_specs = (P(None, "gy", None, "gx", None, "gz"),)
    out_specs = (P(None, "gx", "gy", "gz"), P("gx", "gy", "gz"))
    return jax.shard_map(
        per_device, mesh=mesh, in_specs=in_specs, out_specs=out_specs, check_vma=False
    )
```

```python
import jax
import jax.numpy as jnp
from jax import lax
from jax.experimental import pallas as pl
from jax.experimental.pallas import tpu as pltpu
from jax.sharding import PartitionSpec as P

MESH = pl.DeviceIdType.MESH
F32 = jnp.float32
WIRE = jnp.bfloat16

BASE = 125.5
GAIN = 252.7 / 316.0
SPREAD = 0.05
LOG_SCALE = 1.0 / (GAIN * 0.6931471805599453)


def gauss(offset):
    return jnp.exp(-((offset - 31.5) ** 2) / 128.0)


def filled(scalar, shape):
    return jnp.full(shape, scalar, F32)


def encode(value, dither):
    size = jnp.exp2(jnp.abs(value) * GAIN + dither)
    return jnp.where(value < 0, -size, size).astype(WIRE)


def decode(code, dither):
    code = code.astype(F32)
    size = jnp.log(jnp.abs(code)) * LOG_SCALE - dither * (1.0 / GAIN)
    return jnp.where(code < 0, -size, size)


def share(offset):
    near = gauss(offset)
    return near / (near + gauss(offset + 32.0))


def kernel(
    patches,
    sums,
    side_sums,
    raw,
    packed,
    part,
    partial,
    matrix,
    part_matrix,
    pick,
    own,
    up_same,
    low_cross,
    up_cross,
    got_up_same,
    got_low_cross,
    got_up_cross,
    folded,
    slots,
    dither,
    prob,
    got_block,
    rows,
    corners,
    got_planes,
    got_rows,
    got_corners,
    far_sem,
    load_sem,
    part_sem,
    x_send,
    x_recv,
    z_send,
    z_recv,
    h_send,
    h_recv,
):
    gx, gy, gz = lax.axis_index("gx"), lax.axis_index("gy"), lax.axis_index("gz")
    zc, xl = gx // 2, lax.rem(gx, 2)
    half = zc // 4
    xo = 1 - xl
    gx_by = {1: lax.rem(gx + 1, 16), 0: gx, -1: lax.rem(gx + 15, 16)}
    gy_by = {1: lax.rem(gy + 1, 8), 0: gy, -1: lax.rem(gy + 7, 8)}
    gx_cross = zc * 2 + xo
    partner = (gx, gy, 1 - gz)

    def target(k):
        near_order = jnp.where(k < 3, k + 4, jnp.where(k < 7, k - 3, 7))
        k = jnp.where(half == 1, k, near_order)
        other = (k < 4).astype(jnp.int32)
        step = jnp.where(k == 4, 2, jnp.where(k == 5, 1, jnp.where(k == 6, 3, lax.rem(k, 7))))
        return 4 * lax.rem(half + other, 2) + lax.rem(zc + step, 4)

    def load(k, side):
        a = jnp.maximum(2 * target(k) + (xl if side == 0 else xo) - half, 0)
        return pltpu.make_async_copy(
            patches.at[a, 0], raw.at[2 * k + side], load_sem.at[2 * k + side]
        )

    def start_loads(k, _):
        load(k, 1).start()
        load(k, 0).start()
        return 0

    lax.fori_loop(0, 8, start_loads, 0)

    there_x = {1: gx < 15, 0: gx >= 0, -1: gx > 0}
    there_y = {1: gy < 7, 0: gy >= 0, -1: gy > 0}
    around = [(i, j) for i in (-1, 0, 1) for j in (-1, 0, 1) if i or j]
    barrier = pltpu.get_barrier_semaphore()
    pl.semaphore_signal(barrier, inc=1, device_id=partner, device_id_type=MESH)
    for i, j in around:

        @pl.when(there_x[i] & there_y[j])
        def _():
            for to in (gz, 1 - gz):
                peer = (gx_by[i], gy_by[j], to)
                pl.semaphore_signal(barrier, inc=1, device_id=peer, device_id_type=MESH)

    for d in range(1, 4):
        peer = (2 * (4 * half + lax.rem(zc + d, 4)) + xl, gy, gz)
        pl.semaphore_signal(barrier, inc=1, device_id=peer, device_id_type=MESH)

    @pl.when(half == 0)
    def _():
        for d in range(4, 8):
            peer = (2 * d + xl, gy, gz)
            pl.semaphore_signal(barrier, inc=1, device_id=peer, device_id_type=MESH)

    wide_x = 3 - (gx == 0).astype(jnp.int32) - (gx == 15).astype(jnp.int32)
    wide_y = 3 - (gy == 0).astype(jnp.int32) - (gy == 7).astype(jnp.int32)
    arrivals = 2 * (wide_x * wide_y - 1) + 1 + 3 + 4 * half

    cell = lax.broadcasted_iota(jnp.int32, (128, 256), 0)
    lane = lax.rem(lax.broadcasted_iota(jnp.int32, (128, 256), 1), 128)
    leading = lax.broadcasted_iota(jnp.int32, (128, 256), 1) < 128
    upper = filled(gz.astype(F32), (128, 256))

    def two_terms(value):
        head = value.astype(WIRE).astype(F32)
        return jnp.where(leading, head, value - head).astype(WIRE)

    inner = lax.rem(cell, 32).astype(F32)
    weight = gauss(lax.rem(cell, 64).astype(F32)) / (gauss(inner) + gauss(inner + 32.0))
    weight = jnp.where((cell < 32) & (upper < 0.5), 1.0, weight)
    place = jnp.where(cell < 64, cell, cell - 32)
    hit = (place == lax.rem(lane, 64)) & (cell < 96)
    second = lane >= 64
    weight = jnp.where(hit, weight, 0.0)
    matrix[0:128] = two_terms(-weight)
    matrix[128:256] = two_terms(jnp.where(second, 0.0, weight))
    matrix[256:384] = two_terms(jnp.where(second, weight, 0.0))
    weight = 1.0 - share(inner)
    weight = jnp.where(lax.rem(cell, 32) == lax.rem(lane, 64), weight, 0.0)
    chosen = jnp.where(second, 2, 1) == cell // 32
    weight = jnp.where(cell < 32, -weight, jnp.where(chosen, weight, 0.0))
    part_matrix[...] = two_terms(weight)
    for c in range(3):
        to = lax.broadcasted_iota(jnp.int32, (128, 128), 1) - 32 * c
        at = lax.broadcasted_iota(jnp.int32, (128, 128), 0) - 96
        pick[128 * c : 128 * c + 128] = jnp.where((at == to) & (at >= 0), 1.0, 0.0).astype(WIRE)

    number = lax.broadcasted_iota(jnp.int32, (32, 128), 0) * 128 + lax.broadcasted_iota(
        jnp.int32, (32, 128), 1
    )
    for u in range(8):
        mixed = (number + 4096 * u + 1) * -1640531535
        mixed = (mixed ^ lax.shift_right_logical(mixed, 15)) * -2048144789
        mixed = (mixed ^ lax.shift_right_logical(mixed, 13)) * -1028477387
        bits = lax.shift_right_logical(mixed, 8) & 1023
        dither[u] = bits.astype(F32) * (SPREAD / 1024.0) - BASE

    def send_part(k, side):
        return pltpu.make_async_remote_copy(
            src_ref=packed.at[2 * k + side],
            dst_ref=part.at[2 * k + side],
            send_sem=part_sem.at[0, 2 * k + side],
            recv_sem=part_sem.at[1, 2 * k + side],
            device_id=partner,
            device_id_type=MESH,
        )

    def x_copies(k):
        t = target(k)
        plan = (
            (low_cross, got_low_cross, (gx_cross, gy, gz)),
            (up_cross, got_up_cross, (gx_cross, gy_by[1], gz)),
            (up_same, got_up_same, (gx, gy_by[1], gz)),
        )
        return [
            pltpu.make_async_remote_copy(
                src_ref=src.at[t],
                dst_ref=dst.at[t],
                send_sem=x_send.at[i, t],
                recv_sem=x_recv.at[i, t],
                device_id=device,
                device_id_type=MESH,
            )
            for i, (src, dst, device) in enumerate(plan)
        ]

    def cells(k, side):
        classes = [raw[2 * k + side, c].reshape(256, 128) for c in range(3)]
        return jnp.concatenate(classes, axis=1)

    def product(left, right):
        both = jnp.dot(left, right[...], preferred_element_type=F32)
        return both[:, :128] + both[:, 128:]

    def emit(k, side, d):
        t = target(k)
        for u in range(4):
            low, high = d[64 * u : 64 * u + 32], d[64 * u + 32 : 64 * u + 64]
            if side == 0:
                own[t, u] = low
                up_same[t, u] = encode(high, dither[u])
            else:
                low_cross[t, u] = encode(low, dither[u])
                up_cross[t, u] = encode(high, dither[u])

    pl.semaphore_wait(barrier, arrivals)

    @pl.when(half == 1)
    def _():
        for d in range(4):
            peer = (2 * d + xl, gy, gz)
            pl.semaphore_signal(far_sem, inc=1, device_id=peer, device_id_type=MESH)

    def start_x(k):
        low, *high = x_copies(k)
        low.start()

        @pl.when(gy < 7)
        def _():
            for copy in high:
                copy.start()

    def fold_first(k, _):
        for side in (1, 0):
            load(k, side).wait()
            picked = jnp.dot(cells(k, side), pick[...], preferred_element_type=F32)
            packed[2 * k + side] = picked.astype(WIRE)
            send_part(k, side).start()
        for side in (1, 0):
            emit(k, side, product(cells(k, side), matrix))
        start_x(k)
        return 0

    def fold_second(k, _):
        for side in (1, 0):
            load(k, side).wait()
            partial[side] = product(cells(k, side), matrix)
        for side in (1, 0):
            send_part(k, side).wait_recv()
            more = product(part[2 * k + side], part_matrix)
            emit(k, side, partial[side] + more)
        start_x(k)
        return 0

    lax.fori_loop(0, 8 * (1 - gz), fold_first, 0)
    lax.fori_loop(0, 8 * gz, fold_second, 0)

    cell = lax.broadcasted_iota(jnp.int32, (32, 128), 0)
    has_below = filled((gy > 0).astype(F32), (32, 128)) > 0.5
    high_y = 1.0 - share(cell.astype(F32))

    def z_copy(k):
        t = target(k)
        return pltpu.make_async_remote_copy(
            src_ref=folded.at[t],
            dst_ref=slots.at[zc],
            send_sem=z_send.at[t],
            recv_sem=z_recv.at[zc],
            device_id=(2 * t + xl, gy, gz),
            device_id_type=MESH,
        )

    def forward(k, dst, place):
        t = target(k)
        low, *high = x_copies(k)
        low.wait_recv()

        @pl.when(gy > 0)
        def _():
            for copy in high:
                copy.wait_recv()

        for u in range(4):
            same = own[t, u]
            more = high_y * (decode(got_up_same[t, u], dither[u]) - same)
            same += jnp.where(has_below, more, 0.0)
            cross = decode(got_low_cross[t, u], dither[u])
            more = high_y * (decode(got_up_cross[t, u], dither[u]) - cross)
            cross += jnp.where(has_below, more, 0.0)
            dst[place, 4 * xl + u] = encode(same, dither[4 + u])
            dst[place, 4 * xo + u] = encode(cross, dither[4 + u])

    def pass_on(k, _):
        forward(k, folded, target(k))
        z_copy(k).start()
        return 0

    lax.fori_loop(0, 3, pass_on, 0)

    @pl.when(half == 0)
    def _():
        pl.semaphore_wait(far_sem, 4)

    lax.fori_loop(3, 7, pass_on, 0)
    forward(jnp.int32(7), slots, zc)

    def await_slot(s):
        @pl.when(zc != s)
        def _():
            pltpu.make_async_remote_copy(
                src_ref=folded.at[0],
                dst_ref=slots.at[s],
                send_sem=z_send.at[0],
                recv_sem=z_recv.at[s],
                device_id=partner,
                device_id_type=MESH,
            ).wait_recv()

    has_before = (gx >= 1).astype(F32)

    def softmax(s, _):
        await_slot(s)
        await_slot(s + 4)
        for i in range(8):
            x = 8 * s + i
            high_x = (1.0 - share(filled(x.astype(F32), (1, 128)))) * has_before
            near = decode(slots[s, i], dither[4 + i % 4])
            far = decode(slots[s + 4, i], dither[4 + i % 4])
            d = near + high_x * (far - near)
            top = jnp.maximum(jnp.maximum(d, pltpu.roll(d, 64, 1)), 0.0)
            e = jnp.exp(d - top)
            p = e / (e + pltpu.roll(e, 64, 1) + jnp.exp(-top))
            prob[x] = p
            rows[0, pl.ds(x, 1)] = p[0:1]
            rows[1, pl.ds(x, 1)] = p[31:32]
        return 0

    lax.fori_loop(0, 4, softmax, 0)
    for i in range(2):
        for j in range(2):
            corners[2 * i + j] = rows[j, 31 * i : 31 * i + 1]

    halos = []

    def exchange(src, dst, i, j, to):
        n = len(halos)
        copy = pltpu.make_async_remote_copy(
            src_ref=src,
            dst_ref=dst,
            send_sem=h_send.at[n],
            recv_sem=h_recv.at[n],
            device_id=(gx_by[i], gy_by[j], to),
            device_id_type=MESH,
        )
        out, back = there_x[i] & there_y[j], there_x[-i] & there_y[-j]
        halos.append((copy, out, back))
        pl.when(out)(copy.start)

    for other in range(2):
        to = 1 - gz if other else gz
        for i in range(2):
            for j in range(2):
                exchange(
                    corners.at[2 * i + j],
                    got_corners.at[other, 2 * (1 - i) + 1 - j],
                    2 * i - 1,
                    2 * j - 1,
                    to,
                )
    for other in range(2):
        to = 1 - gz if other else gz
        for i in range(2):
            exchange(rows.at[i], got_rows.at[other, 1 - i], 0, 2 * i - 1, to)
        for i in range(2):
            exchange(prob.at[31 * i], got_planes.at[other, 1 - i], 2 * i - 1, 0, to)
    exchange(prob, got_block, 0, 0, 1 - gz)

    def sum_z(p, q):
        at = lax.rem(lax.broadcasted_iota(jnp.int32, p.shape, 1), 64)
        upper = filled(gz.astype(F32), p.shape)
        edge = pltpu.roll(q, 63 + 2 * gz, 1)
        before = jnp.where(at == 0, edge * upper, pltpu.roll(p, 1, 1))
        after = jnp.where(at == 63, edge * (1.0 - upper), pltpu.roll(p, 127, 1))
        return before + p + after

    halos[-1][0].wait_recv()

    def sum_block(s, _):
        for i in range(4):
            sums[4 * s + i + 1] = sum_z(prob[4 * s + i], got_block[4 * s + i])
        return 0

    lax.fori_loop(0, 8, sum_block, 0)
    for copy, _, back in halos[:-1]:
        pl.when(back)(copy.wait_recv)

    def inside(value, condition):
        return jnp.where(filled(condition.astype(F32), value.shape) > 0.5, value, 0.0)

    for i in range(2):
        here = there_x[2 * i - 1]
        sums[33 * i] = inside(sum_z(got_planes[0, i], got_planes[1, i]), here)
    for j in range(2):
        here = there_y[2 * j - 1]
        side_sums[j, 1:33] = inside(sum_z(got_rows[0, j], got_rows[1, j]), here)
        for i in range(2):
            n = 2 * i + j
            corner = sum_z(
                jnp.broadcast_to(got_corners[0, n], (8, 128)),
                jnp.broadcast_to(got_corners[1, n], (8, 128)),
            )
            here = there_x[2 * i - 1] & there_y[2 * j - 1]
            side_sums[j, 33 * i : 33 * i + 1] = inside(corner, here)[0:1]

    @pl.when(gz == 0)
    def _():
        def finish(k, _):
            send_part(k, 0).wait_send()
            send_part(k, 1).wait_send()
            return 0

        lax.fori_loop(0, 8, finish, 0)

    def finish(k, _):
        low, *high = x_copies(k)
        low.wait_send()

        @pl.when(gy < 7)
        def _():
            for copy in high:
                copy.wait_send()

        return 0

    lax.fori_loop(0, 8, finish, 0)

    def finish_z(k, _):
        z_copy(k).wait_send()
        return 0

    lax.fori_loop(0, 7, finish_z, 0)
    for copy, out, _ in halos:
        pl.when(out)(copy.wait_send)


def box(sums, side_sums, smooth, conf, sides):
    gx, gy, gz = lax.axis_index("gx"), lax.axis_index("gy"), lax.axis_index("gz")
    step = pl.program_id(0)
    count = smooth.shape[1]
    lane = lax.rem(lax.broadcasted_iota(jnp.int32, (32, 128), 1), 64)
    cell = lax.broadcasted_iota(jnp.int32, (32, 128), 0)

    def cut(place, at, there):
        return jnp.where(place == at, filled(there.astype(F32), (32, 128)), 0.0)

    count_y = 3.0 - cut(cell, 0, gy == 0) - cut(cell, 31, gy == 7)
    count_z = 3.0 - cut(lane, 0, gz == 0) - cut(lane, 63, gz == 1)
    inverse = 1.0 / (count_y * count_z)
    for j in range(2):
        sides[j] = side_sums[j, 0:32] + side_sums[j, 1:33] + side_sums[j, 2:34]
    for i in range(count):
        x = step * count + i
        s = sums[x] + sums[x + 1] + sums[x + 2]
        low = jnp.broadcast_to(sides[0, pl.ds(x, 1)], (32, 128))
        high = jnp.broadcast_to(sides[1, pl.ds(x, 1)], (32, 128))
        before = jnp.where(cell == 0, low, pltpu.roll(s, 1, 0))
        after = jnp.where(cell == 31, high, pltpu.roll(s, 31, 0))
        end = ((gx == 0) & (x == 0)) | ((gx == 15) & (x == 31))
        count_x = 3.0 - filled(end.astype(F32), (32, 128))
        s1 = (before + s + after) * (inverse / count_x)
        s2 = pltpu.roll(s1, 64, 1)
        s0 = 1.0 - s1 - s2
        smooth[0, i] = s0[:, :64]
        smooth[1, i] = s1[:, :64]
        smooth[2, i] = s2[:, :64]
        conf[i] = jnp.maximum(jnp.maximum(s0, s1), s2)[:, :64]


def per_device(patches):
    vmem = pltpu.VMEM
    dma = pltpu.SemaphoreType.DMA
    in_hbm = pl.BlockSpec(memory_space=pltpu.HBM)
    in_vmem = pl.BlockSpec(memory_space=pltpu.VMEM)
    sums, side_sums = pl.pallas_call(
        kernel,
        name="stitch",
        out_shape=(
            jax.ShapeDtypeStruct((34, 32, 128), F32),
            jax.ShapeDtypeStruct((2, 40, 128), F32),
        ),
        in_specs=[in_hbm],
        out_specs=(in_vmem, in_vmem),
        scratch_shapes=[
            vmem((16, 3, 4, 64, 128), jnp.bfloat16),
            vmem((16, 256, 128), WIRE),
            vmem((16, 256, 128), WIRE),
            vmem((2, 256, 128), F32),
            vmem((384, 256), WIRE),
            vmem((128, 256), WIRE),
            vmem((384, 128), WIRE),
            vmem((8, 4, 32, 128), F32),
            *[vmem((8, 4, 32, 128), WIRE)] * 6,
            vmem((8, 8, 32, 128), WIRE),
            vmem((8, 8, 32, 128), WIRE),
            vmem((8, 32, 128), F32),
            vmem((32, 32, 128), F32),
            vmem((32, 32, 128), F32),
            vmem((2, 32, 128), F32),
            vmem((4, 1, 128), F32),
            vmem((2, 2, 32, 128), F32),
            vmem((2, 2, 32, 128), F32),
            vmem((2, 4, 1, 128), F32),
            pltpu.SemaphoreType.REGULAR,
            dma((16,)),
            dma((2, 16)),
            dma((3, 8)),
            dma((3, 8)),
            dma((8,)),
            dma((8,)),
            dma((17,)),
            dma((17,)),
        ],
        compiler_params=pltpu.CompilerParams(
            collective_id=0, has_side_effects=True, vmem_limit_bytes=52 << 20
        ),
    )(patches)
    steps = 4
    return pl.pallas_call(
        box,
        name="box",
        grid=(steps,),
        out_shape=(
            jax.ShapeDtypeStruct((3, 32, 32, 64), F32),
            jax.ShapeDtypeStruct((32, 32, 64), F32),
        ),
        in_specs=[in_vmem, in_vmem],
        out_specs=(
            pl.BlockSpec((3, 32 // steps, 32, 64), lambda i: (0, i, 0, 0)),
            pl.BlockSpec((32 // steps, 32, 64), lambda i: (i, 0, 0)),
        ),
        scratch_shapes=[vmem((2, 32, 128), F32)],
        compiler_params=pltpu.CompilerParams(vmem_limit_bytes=20 << 20),
    )(sums, side_sums)


def solution(mesh):
    in_specs = (P(None, "gy", None, "gx", None, "gz"),)
    out_specs = (P(None, "gx", "gy", "gz"), P("gx", "gy", "gz"))
    return jax.shard_map(
        per_device, mesh=mesh, in_specs=in_specs, out_specs=out_specs, check_vma=False
    )
```

```python
import jax
import jax.numpy as jnp
from jax import lax
from jax.experimental import pallas as pl
from jax.experimental.pallas import tpu as pltpu
from jax.sharding import PartitionSpec as P

MESH = pl.DeviceIdType.MESH
F32 = jnp.float32
WIRE = jnp.bfloat16
PARTS = 4

BASE = 125.5
GAIN = 252.7 / 316.0
SPREAD = 0.05
LOG_SCALE = 1.0 / (GAIN * 0.6931471805599453)


def gauss(offset):
    return jnp.exp(-((offset - 31.5) ** 2) / 128.0)


def filled(scalar, shape):
    return jnp.full(shape, scalar, F32)


def encode(value, dither):
    size = jnp.exp2(jnp.abs(value) * GAIN + dither)
    return jnp.where(value < 0, -size, size).astype(WIRE)


def decode(code, dither):
    code = code.astype(F32)
    size = jnp.log(jnp.abs(code)) * LOG_SCALE - dither * (1.0 / GAIN)
    return jnp.where(code < 0, -size, size)


def share(offset):
    near = gauss(offset)
    return near / (near + gauss(offset + 32.0))


def kernel(
    patches,
    sums,
    side_sums,
    raw,
    packed,
    part,
    partial,
    matrix,
    part_matrix,
    pick,
    own,
    up_same,
    low_cross,
    up_cross,
    got_up_same,
    got_low_cross,
    got_up_cross,
    folded,
    slots,
    dither,
    prob,
    got_block,
    rows,
    corners,
    got_planes,
    got_rows,
    got_corners,
    far_sem,
    load_sem,
    part_sem,
    x_send,
    x_recv,
    z_send,
    z_recv,
    h_send,
    h_recv,
):
    gx, gy, gz = lax.axis_index("gx"), lax.axis_index("gy"), lax.axis_index("gz")
    zc, xl = gx // 2, lax.rem(gx, 2)
    half = zc // 4
    xo = 1 - xl
    gx_by = {1: lax.rem(gx + 1, 16), 0: gx, -1: lax.rem(gx + 15, 16)}
    gy_by = {1: lax.rem(gy + 1, 8), 0: gy, -1: lax.rem(gy + 7, 8)}
    gx_cross = zc * 2 + xo
    partner = (gx, gy, 1 - gz)

    def target(k):
        near_order = jnp.where(k < 3, k + 4, jnp.where(k < 7, k - 3, 7))
        k = jnp.where(half == 1, k, near_order)
        other = (k < 4).astype(jnp.int32)
        step = jnp.where(k == 4, 2, jnp.where(k == 5, 1, jnp.where(k == 6, 3, lax.rem(k, 7))))
        return 4 * lax.rem(half + other, 2) + lax.rem(zc + step, 4)

    def load(k, side):
        a = jnp.maximum(2 * target(k) + (xl if side == 0 else xo) - half, 0)
        return pltpu.make_async_copy(
            patches.at[a, 0], raw.at[2 * k + side], load_sem.at[2 * k + side]
        )

    def start_loads(k, _):
        load(k, 1).start()
        load(k, 0).start()
        return 0

    start_loads(jnp.int32(0), 0)

    there_x = {1: gx < 15, 0: gx >= 0, -1: gx > 0}
    there_y = {1: gy < 7, 0: gy >= 0, -1: gy > 0}
    around = [(i, j) for i in (-1, 0, 1) for j in (-1, 0, 1) if i or j]
    barrier = pltpu.get_barrier_semaphore()
    pl.semaphore_signal(barrier, inc=1, device_id=partner, device_id_type=MESH)
    for i, j in around:

        @pl.when(there_x[i] & there_y[j])
        def _():
            for to in (gz, 1 - gz):
                peer = (gx_by[i], gy_by[j], to)
                pl.semaphore_signal(barrier, inc=1, device_id=peer, device_id_type=MESH)

    for d in range(1, 4):
        peer = (2 * (4 * half + lax.rem(zc + d, 4)) + xl, gy, gz)
        pl.semaphore_signal(barrier, inc=1, device_id=peer, device_id_type=MESH)

    @pl.when(half == 0)
    def _():
        for d in range(4, 8):
            peer = (2 * d + xl, gy, gz)
            pl.semaphore_signal(barrier, inc=1, device_id=peer, device_id_type=MESH)

    wide_x = 3 - (gx == 0).astype(jnp.int32) - (gx == 15).astype(jnp.int32)
    wide_y = 3 - (gy == 0).astype(jnp.int32) - (gy == 7).astype(jnp.int32)
    arrivals = 2 * (wide_x * wide_y - 1) + 1 + 3 + 4 * half

    cell = lax.broadcasted_iota(jnp.int32, (128, 256), 0)
    lane = lax.rem(lax.broadcasted_iota(jnp.int32, (128, 256), 1), 128)
    leading = lax.broadcasted_iota(jnp.int32, (128, 256), 1) < 128
    upper = filled(gz.astype(F32), (128, 256))

    def two_terms(value):
        head = value.astype(WIRE).astype(F32)
        return jnp.where(leading, head, value - head).astype(WIRE)

    inner = lax.rem(cell, 32).astype(F32)
    weight = gauss(lax.rem(cell, 64).astype(F32)) / (gauss(inner) + gauss(inner + 32.0))
    weight = jnp.where((cell < 32) & (upper < 0.5), 1.0, weight)
    place = jnp.where(cell < 64, cell, cell - 32)
    hit = (place == lax.rem(lane, 64)) & (cell < 96)
    second = lane >= 64
    weight = jnp.where(hit, weight, 0.0)
    matrix[0:128] = two_terms(-weight)
    matrix[128:256] = two_terms(jnp.where(second, 0.0, weight))
    matrix[256:384] = two_terms(jnp.where(second, weight, 0.0))
    weight = 1.0 - share(inner)
    weight = jnp.where(lax.rem(cell, 32) == lax.rem(lane, 64), weight, 0.0)
    chosen = jnp.where(second, 2, 1) == cell // 32
    weight = jnp.where(cell < 32, -weight, jnp.where(chosen, weight, 0.0))
    part_matrix[...] = two_terms(weight)
    for c in range(3):
        to = lax.broadcasted_iota(jnp.int32, (128, 128), 1) - 32 * c
        at = lax.broadcasted_iota(jnp.int32, (128, 128), 0) - 96
        pick[128 * c : 128 * c + 128] = jnp.where((at == to) & (at >= 0), 1.0, 0.0).astype(WIRE)

    lax.fori_loop(1, 8, start_loads, 0)
    number = lax.broadcasted_iota(jnp.int32, (32, 128), 0) * 128 + lax.broadcasted_iota(
        jnp.int32, (32, 128), 1
    )
    for u in range(8):
        mixed = (number + 4096 * u + 1) * -1640531535
        mixed = (mixed ^ lax.shift_right_logical(mixed, 15)) * -2048144789
        mixed = (mixed ^ lax.shift_right_logical(mixed, 13)) * -1028477387
        bits = lax.shift_right_logical(mixed, 8) & 1023
        dither[u] = bits.astype(F32) * (SPREAD / 1024.0) - BASE

    def send_part(k, side):
        return pltpu.make_async_remote_copy(
            src_ref=packed.at[2 * k + side],
            dst_ref=part.at[2 * k + side],
            send_sem=part_sem.at[0, 2 * k + side],
            recv_sem=part_sem.at[1, 2 * k + side],
            device_id=partner,
            device_id_type=MESH,
        )

    def x_copies(k):
        t = target(k)
        plan = (
            (low_cross, got_low_cross, (gx_cross, gy, gz)),
            (up_cross, got_up_cross, (gx_cross, gy_by[1], gz)),
            (up_same, got_up_same, (gx, gy_by[1], gz)),
        )
        return [
            pltpu.make_async_remote_copy(
                src_ref=src.at[t],
                dst_ref=dst.at[t],
                send_sem=x_send.at[i, t],
                recv_sem=x_recv.at[i, t],
                device_id=device,
                device_id_type=MESH,
            )
            for i, (src, dst, device) in enumerate(plan)
        ]

    def cells(k, side):
        classes = [raw[2 * k + side, c].reshape(256, 128) for c in range(3)]
        return jnp.concatenate(classes, axis=1)

    def product(left, right):
        both = jnp.dot(left, right[...], preferred_element_type=F32)
        return both[:, :128] + both[:, 128:]

    def emit(k, side, d):
        t = target(k)
        for u in range(4):
            low, high = d[64 * u : 64 * u + 32], d[64 * u + 32 : 64 * u + 64]
            if side == 0:
                own[t, u] = low
                up_same[t, u] = encode(high, dither[u])
            else:
                low_cross[t, u] = encode(low, dither[u])
                up_cross[t, u] = encode(high, dither[u])

    pl.semaphore_wait(barrier, arrivals)

    @pl.when(half == 1)
    def _():
        for d in range(4):
            peer = (2 * d + xl, gy, gz)
            pl.semaphore_signal(far_sem, inc=1, device_id=peer, device_id_type=MESH)

    def start_x(k):
        low, *high = x_copies(k)
        low.start()

        @pl.when(gy < 7)
        def _():
            for copy in high:
                copy.start()

    def fold_first(k, _):
        for side in (1, 0):
            load(k, side).wait()
            picked = jnp.dot(cells(k, side), pick[...], preferred_element_type=F32)
            packed[2 * k + side] = picked.astype(WIRE)
            send_part(k, side).start()
        for side in (1, 0):
            emit(k, side, product(cells(k, side), matrix))
        start_x(k)
        return 0

    def fold_second(k, _):
        for side in (1, 0):
            load(k, side).wait()
            partial[side] = product(cells(k, side), matrix)
        for side in (1, 0):
            send_part(k, side).wait_recv()
            more = product(part[2 * k + side], part_matrix)
            emit(k, side, partial[side] + more)
        start_x(k)
        return 0

    cell = lax.broadcasted_iota(jnp.int32, (32, 128), 0)
    has_below = filled((gy > 0).astype(F32), (32, 128)) > 0.5
    high_y = 1.0 - share(cell.astype(F32))

    def z_copy(k):
        t = target(k)
        return pltpu.make_async_remote_copy(
            src_ref=folded.at[t],
            dst_ref=slots.at[zc],
            send_sem=z_send.at[t],
            recv_sem=z_recv.at[zc],
            device_id=(2 * t + xl, gy, gz),
            device_id_type=MESH,
        )

    def forward(k, dst, place):
        t = target(k)
        low, *high = x_copies(k)
        low.wait_recv()

        @pl.when(gy > 0)
        def _():
            for copy in high:
                copy.wait_recv()

        for u in range(4):
            same = own[t, u]
            more = high_y * (decode(got_up_same[t, u], dither[u]) - same)
            same += jnp.where(has_below, more, 0.0)
            cross = decode(got_low_cross[t, u], dither[u])
            more = high_y * (decode(got_up_cross[t, u], dither[u]) - cross)
            cross += jnp.where(has_below, more, 0.0)
            dst[place, 4 * xl + u] = encode(same, dither[4 + u])
            dst[place, 4 * xo + u] = encode(cross, dither[4 + u])

    def pass_on(k, _):
        @pl.when((half == 0) & (k == 3))
        def _():
            pl.semaphore_wait(far_sem, 4)

        forward(k, folded, target(k))
        z_copy(k).start()
        return 0

    def step(k, _):
        @pl.when(gz == 0)
        def _():
            fold_first(k, 0)

        @pl.when(gz == 1)
        def _():
            fold_second(k, 0)

        @pl.when(k >= 3)
        def _():
            pass_on(k - 3, 0)

        return 0

    lax.fori_loop(0, 8, step, 0)
    lax.fori_loop(5, 7, pass_on, 0)
    forward(jnp.int32(7), slots, zc)

    def await_slot(s):
        @pl.when(zc != s)
        def _():
            pltpu.make_async_remote_copy(
                src_ref=folded.at[0],
                dst_ref=slots.at[s],
                send_sem=z_send.at[0],
                recv_sem=z_recv.at[s],
                device_id=partner,
                device_id_type=MESH,
            ).wait_recv()

    has_before = (gx >= 1).astype(F32)

    def softmax(s, _):
        await_slot(s)
        await_slot(s + 4)
        for i in range(8):
            x = 8 * s + i
            high_x = (1.0 - share(filled(x.astype(F32), (1, 128)))) * has_before
            near = decode(slots[s, i], dither[4 + i % 4])
            far = decode(slots[s + 4, i], dither[4 + i % 4])
            d = near + high_x * (far - near)
            top = jnp.maximum(jnp.maximum(d, pltpu.roll(d, 64, 1)), 0.0)
            e = jnp.exp(d - top)
            p = e / (e + pltpu.roll(e, 64, 1) + jnp.exp(-top))
            prob[x] = p
            rows[0, pl.ds(x, 1)] = p[0:1]
            rows[1, pl.ds(x, 1)] = p[31:32]
        return 0

    lax.fori_loop(0, 4, softmax, 0)
    for i in range(2):
        for j in range(2):
            corners[2 * i + j] = rows[j, 31 * i : 31 * i + 1]

    halos = []

    def exchange(src, dst, i, j, to):
        n = len(halos)
        copy = pltpu.make_async_remote_copy(
            src_ref=src,
            dst_ref=dst,
            send_sem=h_send.at[n],
            recv_sem=h_recv.at[n],
            device_id=(gx_by[i], gy_by[j], to),
            device_id_type=MESH,
        )
        out, back = there_x[i] & there_y[j], there_x[-i] & there_y[-j]
        halos.append((copy, out, back))
        pl.when(out)(copy.start)

    for other in range(2):
        to = 1 - gz if other else gz
        for i in range(2):
            for j in range(2):
                exchange(
                    corners.at[2 * i + j],
                    got_corners.at[other, 2 * (1 - i) + 1 - j],
                    2 * i - 1,
                    2 * j - 1,
                    to,
                )
    for other in range(2):
        to = 1 - gz if other else gz
        for i in range(2):
            exchange(rows.at[i], got_rows.at[other, 1 - i], 0, 2 * i - 1, to)
        for i in range(2):
            exchange(prob.at[31 * i], got_planes.at[other, 1 - i], 2 * i - 1, 0, to)
    exchange(prob, got_block, 0, 0, 1 - gz)

    def sum_z(p, q):
        at = lax.rem(lax.broadcasted_iota(jnp.int32, p.shape, 1), 64)
        upper = filled(gz.astype(F32), p.shape)
        edge = pltpu.roll(q, 63 + 2 * gz, 1)
        before = jnp.where(at == 0, edge * upper, pltpu.roll(p, 1, 1))
        after = jnp.where(at == 63, edge * (1.0 - upper), pltpu.roll(p, 127, 1))
        return before + p + after

    halos[-1][0].wait_recv()

    def sum_block(s, _):
        for i in range(4):
            sums[4 * s + i + 1] = sum_z(prob[4 * s + i], got_block[4 * s + i])
        return 0

    lax.fori_loop(0, 8, sum_block, 0)
    for copy, _, back in halos[:-1]:
        pl.when(back)(copy.wait_recv)

    def inside(value, condition):
        return jnp.where(filled(condition.astype(F32), value.shape) > 0.5, value, 0.0)

    for i in range(2):
        here = there_x[2 * i - 1]
        sums[33 * i] = inside(sum_z(got_planes[0, i], got_planes[1, i]), here)
    for j in range(2):
        here = there_y[2 * j - 1]
        side_sums[j, 1:33] = inside(sum_z(got_rows[0, j], got_rows[1, j]), here)
        for i in range(2):
            n = 2 * i + j
            corner = sum_z(
                jnp.broadcast_to(got_corners[0, n], (8, 128)),
                jnp.broadcast_to(got_corners[1, n], (8, 128)),
            )
            here = there_x[2 * i - 1] & there_y[2 * j - 1]
            side_sums[j, 33 * i : 33 * i + 1] = inside(corner, here)[0:1]

    @pl.when(gz == 0)
    def _():
        def finish(k, _):
            send_part(k, 0).wait_send()
            send_part(k, 1).wait_send()
            return 0

        lax.fori_loop(0, 8, finish, 0)

    def finish(k, _):
        low, *high = x_copies(k)
        low.wait_send()

        @pl.when(gy < 7)
        def _():
            for copy in high:
                copy.wait_send()

        return 0

    lax.fori_loop(0, 8, finish, 0)

    def finish_z(k, _):
        z_copy(k).wait_send()
        return 0

    lax.fori_loop(0, 7, finish_z, 0)
    for copy, out, _ in halos:
        pl.when(out)(copy.wait_send)


def box(sums, side_sums, smooth, conf, sides, smooth_block, conf_block, sems):
    gx, gy, gz = lax.axis_index("gx"), lax.axis_index("gy"), lax.axis_index("gz")
    lane = lax.rem(lax.broadcasted_iota(jnp.int32, (32, 128), 1), 64)
    cell = lax.broadcasted_iota(jnp.int32, (32, 128), 0)

    def cut(place, at, there):
        return jnp.where(place == at, filled(there.astype(F32), (32, 128)), 0.0)

    count_y = 3.0 - cut(cell, 0, gy == 0) - cut(cell, 31, gy == 7)
    count_z = 3.0 - cut(lane, 0, gz == 0) - cut(lane, 63, gz == 1)
    inverse = 1.0 / (count_y * count_z)
    for j in range(2):
        sides[j] = side_sums[j, 0:32] + side_sums[j, 1:33] + side_sums[j, 2:34]

    def plane(x):
        s = sums[x] + sums[x + 1] + sums[x + 2]
        low = jnp.broadcast_to(sides[0, pl.ds(x, 1)], (32, 128))
        high = jnp.broadcast_to(sides[1, pl.ds(x, 1)], (32, 128))
        before = jnp.where(cell == 0, low, pltpu.roll(s, 1, 0))
        after = jnp.where(cell == 31, high, pltpu.roll(s, 31, 0))
        end = ((gx == 0) & (x == 0)) | ((gx == 15) & (x == 31))
        count_x = 3.0 - filled(end.astype(F32), (32, 128))
        s1 = (before + s + after) * (inverse / count_x)
        s2 = pltpu.roll(s1, 64, 1)
        s0 = 1.0 - s1 - s2
        smooth_block[0, x] = s0[:, :64]
        smooth_block[1, x] = s1[:, :64]
        smooth_block[2, x] = s2[:, :64]
        conf_block[x] = jnp.maximum(jnp.maximum(s0, s1), s2)[:, :64]

    def copies(n):
        part = pl.ds(n * (32 // PARTS), 32 // PARTS)
        return (
            pltpu.make_async_copy(smooth_block.at[:, part], smooth.at[:, part], sems.at[0, n]),
            pltpu.make_async_copy(conf_block.at[part], conf.at[part], sems.at[1, n]),
        )

    for n in range(PARTS):

        def some(x, _):
            for i in range(4):
                plane(4 * x + i)
            return 0

        lax.fori_loop(n * (8 // PARTS), (n + 1) * (8 // PARTS), some, 0)
        for copy in copies(n):
            copy.start()
    for n in range(PARTS):
        for copy in copies(n):
            copy.wait()


def per_device(patches):
    vmem = pltpu.VMEM
    dma = pltpu.SemaphoreType.DMA
    in_hbm = pl.BlockSpec(memory_space=pltpu.HBM)
    in_vmem = pl.BlockSpec(memory_space=pltpu.VMEM)
    sums, side_sums = pl.pallas_call(
        kernel,
        name="stitch",
        out_shape=(
            jax.ShapeDtypeStruct((34, 32, 128), F32),
            jax.ShapeDtypeStruct((2, 40, 128), F32),
        ),
        in_specs=[in_hbm],
        out_specs=(in_vmem, in_vmem),
        scratch_shapes=[
            vmem((16, 3, 4, 64, 128), jnp.bfloat16),
            vmem((16, 256, 128), WIRE),
            vmem((16, 256, 128), WIRE),
            vmem((2, 256, 128), F32),
            vmem((384, 256), WIRE),
            vmem((128, 256), WIRE),
            vmem((384, 128), WIRE),
            vmem((8, 4, 32, 128), F32),
            *[vmem((8, 4, 32, 128), WIRE)] * 6,
            vmem((8, 8, 32, 128), WIRE),
            vmem((8, 8, 32, 128), WIRE),
            vmem((8, 32, 128), F32),
            vmem((32, 32, 128), F32),
            vmem((32, 32, 128), F32),
            vmem((2, 32, 128), F32),
            vmem((4, 1, 128), F32),
            vmem((2, 2, 32, 128), F32),
            vmem((2, 2, 32, 128), F32),
            vmem((2, 4, 1, 128), F32),
            pltpu.SemaphoreType.REGULAR,
            dma((16,)),
            dma((2, 16)),
            dma((3, 8)),
            dma((3, 8)),
            dma((8,)),
            dma((8,)),
            dma((17,)),
            dma((17,)),
        ],
        compiler_params=pltpu.CompilerParams(
            collective_id=0, has_side_effects=True, vmem_limit_bytes=52 << 20
        ),
    )(patches)
    return pl.pallas_call(
        box,
        name="box",
        out_shape=(
            jax.ShapeDtypeStruct((3, 32, 32, 64), F32),
            jax.ShapeDtypeStruct((32, 32, 64), F32),
        ),
        in_specs=[in_vmem, in_vmem],
        out_specs=(in_hbm, in_hbm),
        scratch_shapes=[
            vmem((2, 32, 128), F32),
            vmem((3, 32, 32, 64), F32),
            vmem((32, 32, 64), F32),
            dma((2, PARTS)),
        ],
        compiler_params=pltpu.CompilerParams(vmem_limit_bytes=20 << 20),
    )(sums, side_sums)


def solution(mesh):
    in_specs = (P(None, "gy", None, "gx", None, "gz"),)
    out_specs = (P(None, "gx", "gy", "gz"), P("gx", "gy", "gz"))
    return jax.shard_map(
        per_device, mesh=mesh, in_specs=in_specs, out_specs=out_specs, check_vma=False
    )
```

```python
import jax
import jax.numpy as jnp
from jax import lax
from jax.experimental import pallas as pl
from jax.experimental.pallas import tpu as pltpu
from jax.sharding import PartitionSpec as P

MESH = pl.DeviceIdType.MESH
F32 = jnp.float32
WIRE = jnp.bfloat16
PARTS = 4

BASE = 125.5
GAIN = 252.7 / 316.0
SPREAD = 0.05
LOG_SCALE = 1.0 / (GAIN * 0.6931471805599453)


def gauss(offset):
    return jnp.exp(-((offset - 31.5) ** 2) / 128.0)


def filled(scalar, shape):
    return jnp.full(shape, scalar, F32)


def encode(value, dither):
    size = jnp.exp2(jnp.abs(value) * GAIN + dither)
    return jnp.where(value < 0, -size, size).astype(WIRE)


def decode(code, dither):
    code = code.astype(F32)
    size = jnp.log(jnp.abs(code)) * LOG_SCALE - dither * (1.0 / GAIN)
    return jnp.where(code < 0, -size, size)


def share(offset):
    near = gauss(offset)
    return near / (near + gauss(offset + 32.0))


def kernel(
    patches,
    sums,
    side_sums,
    raw,
    packed,
    part,
    partial,
    matrix,
    part_matrix,
    pick,
    own,
    up_same,
    low_cross,
    up_cross,
    got_up_same,
    got_low_cross,
    got_up_cross,
    folded,
    slots,
    dither,
    prob,
    block,
    got_block,
    rows,
    sent_rows,
    corners,
    got_planes,
    got_rows,
    got_corners,
    far_sem,
    load_sem,
    part_sem,
    x_send,
    x_recv,
    z_send,
    z_recv,
    h_send,
    h_recv,
):
    gx, gy, gz = lax.axis_index("gx"), lax.axis_index("gy"), lax.axis_index("gz")
    zc, xl = gx // 2, lax.rem(gx, 2)
    half = zc // 4
    xo = 1 - xl
    gx_by = {1: lax.rem(gx + 1, 16), 0: gx, -1: lax.rem(gx + 15, 16)}
    gy_by = {1: lax.rem(gy + 1, 8), 0: gy, -1: lax.rem(gy + 7, 8)}
    gx_cross = zc * 2 + xo
    partner = (gx, gy, 1 - gz)

    def target(k):
        near_order = jnp.where(k < 3, k + 4, jnp.where(k < 7, k - 3, 7))
        k = jnp.where(half == 1, k, near_order)
        other = (k < 4).astype(jnp.int32)
        step = jnp.where(k == 4, 2, jnp.where(k == 5, 1, jnp.where(k == 6, 3, lax.rem(k, 7))))
        return 4 * lax.rem(half + other, 2) + lax.rem(zc + step, 4)

    def load(k, side):
        a = jnp.maximum(2 * target(k) + (xl if side == 0 else xo) - half, 0)
        return pltpu.make_async_copy(
            patches.at[a, 0], raw.at[2 * k + side], load_sem.at[2 * k + side]
        )

    def start_loads(k, _):
        load(k, 1).start()
        load(k, 0).start()
        return 0

    start_loads(jnp.int32(0), 0)

    there_x = {1: gx < 15, 0: gx >= 0, -1: gx > 0}
    there_y = {1: gy < 7, 0: gy >= 0, -1: gy > 0}
    around = [(i, j) for i in (-1, 0, 1) for j in (-1, 0, 1) if i or j]
    barrier = pltpu.get_barrier_semaphore()
    pl.semaphore_signal(barrier, inc=1, device_id=partner, device_id_type=MESH)
    for i, j in around:

        @pl.when(there_x[i] & there_y[j])
        def _():
            for to in (gz, 1 - gz):
                peer = (gx_by[i], gy_by[j], to)
                pl.semaphore_signal(barrier, inc=1, device_id=peer, device_id_type=MESH)

    for d in range(1, 4):
        peer = (2 * (4 * half + lax.rem(zc + d, 4)) + xl, gy, gz)
        pl.semaphore_signal(barrier, inc=1, device_id=peer, device_id_type=MESH)

    @pl.when(half == 0)
    def _():
        for d in range(4, 8):
            peer = (2 * d + xl, gy, gz)
            pl.semaphore_signal(barrier, inc=1, device_id=peer, device_id_type=MESH)

    wide_x = 3 - (gx == 0).astype(jnp.int32) - (gx == 15).astype(jnp.int32)
    wide_y = 3 - (gy == 0).astype(jnp.int32) - (gy == 7).astype(jnp.int32)
    arrivals = 2 * (wide_x * wide_y - 1) + 1 + 3 + 4 * half

    cell = lax.broadcasted_iota(jnp.int32, (128, 256), 0)
    lane = lax.rem(lax.broadcasted_iota(jnp.int32, (128, 256), 1), 128)
    leading = lax.broadcasted_iota(jnp.int32, (128, 256), 1) < 128
    upper = filled(gz.astype(F32), (128, 256))

    def two_terms(value):
        head = value.astype(WIRE).astype(F32)
        return jnp.where(leading, head, value - head).astype(WIRE)

    inner = lax.rem(cell, 32).astype(F32)
    weight = gauss(lax.rem(cell, 64).astype(F32)) / (gauss(inner) + gauss(inner + 32.0))
    weight = jnp.where((cell < 32) & (upper < 0.5), 1.0, weight)
    place = jnp.where(cell < 64, cell, cell - 32)
    hit = (place == lax.rem(lane, 64)) & (cell < 96)
    second = lane >= 64
    weight = jnp.where(hit, weight, 0.0)
    matrix[0:128] = two_terms(-weight)
    matrix[128:256] = two_terms(jnp.where(second, 0.0, weight))
    matrix[256:384] = two_terms(jnp.where(second, weight, 0.0))
    weight = 1.0 - share(inner)
    weight = jnp.where(lax.rem(cell, 32) == lax.rem(lane, 64), weight, 0.0)
    chosen = jnp.where(second, 2, 1) == cell // 32
    weight = jnp.where(cell < 32, -weight, jnp.where(chosen, weight, 0.0))
    part_matrix[...] = two_terms(weight)
    for c in range(3):
        to = lax.broadcasted_iota(jnp.int32, (128, 128), 1) - 32 * c
        at = lax.broadcasted_iota(jnp.int32, (128, 128), 0) - 96
        pick[128 * c : 128 * c + 128] = jnp.where((at == to) & (at >= 0), 1.0, 0.0).astype(WIRE)

    lax.fori_loop(1, 8, start_loads, 0)
    number = lax.broadcasted_iota(jnp.int32, (32, 128), 0) * 128 + lax.broadcasted_iota(
        jnp.int32, (32, 128), 1
    )
    for u in range(8):
        mixed = (number + 4096 * u + 1) * -1640531535
        mixed = (mixed ^ lax.shift_right_logical(mixed, 15)) * -2048144789
        mixed = (mixed ^ lax.shift_right_logical(mixed, 13)) * -1028477387
        bits = lax.shift_right_logical(mixed, 8) & 1023
        dither[u] = bits.astype(F32) * (SPREAD / 1024.0) - BASE

    def send_part(k, side):
        return pltpu.make_async_remote_copy(
            src_ref=packed.at[2 * k + side],
            dst_ref=part.at[2 * k + side],
            send_sem=part_sem.at[0, 2 * k + side],
            recv_sem=part_sem.at[1, 2 * k + side],
            device_id=partner,
            device_id_type=MESH,
        )

    def x_copies(k):
        t = target(k)
        plan = (
            (low_cross, got_low_cross, (gx_cross, gy, gz)),
            (up_cross, got_up_cross, (gx_cross, gy_by[1], gz)),
            (up_same, got_up_same, (gx, gy_by[1], gz)),
        )
        return [
            pltpu.make_async_remote_copy(
                src_ref=src.at[t],
                dst_ref=dst.at[t],
                send_sem=x_send.at[i, t],
                recv_sem=x_recv.at[i, t],
                device_id=device,
                device_id_type=MESH,
            )
            for i, (src, dst, device) in enumerate(plan)
        ]

    def cells(k, side):
        classes = [raw[2 * k + side, c].reshape(256, 128) for c in range(3)]
        return jnp.concatenate(classes, axis=1)

    def product(left, right):
        both = jnp.dot(left, right[...], preferred_element_type=F32)
        return both[:, :128] + both[:, 128:]

    def emit(k, side, d):
        t = target(k)
        for u in range(4):
            low, high = d[64 * u : 64 * u + 32], d[64 * u + 32 : 64 * u + 64]
            if side == 0:
                own[t, u] = low
                up_same[t, u] = encode(high, dither[u])
            else:
                low_cross[t, u] = encode(low, dither[u])
                up_cross[t, u] = encode(high, dither[u])

    pl.semaphore_wait(barrier, arrivals)

    @pl.when(half == 1)
    def _():
        for d in range(4):
            peer = (2 * d + xl, gy, gz)
            pl.semaphore_signal(far_sem, inc=1, device_id=peer, device_id_type=MESH)

    def start_x(k):
        low, *high = x_copies(k)
        low.start()

        @pl.when(gy < 7)
        def _():
            for copy in high:
                copy.start()

    def fold_first(k, _):
        for side in (1, 0):
            load(k, side).wait()
            picked = jnp.dot(cells(k, side), pick[...], preferred_element_type=F32)
            packed[2 * k + side] = picked.astype(WIRE)
            send_part(k, side).start()
        for side in (1, 0):
            emit(k, side, product(cells(k, side), matrix))
        start_x(k)
        return 0

    def fold_second(k, _):
        for side in (1, 0):
            load(k, side).wait()
            partial[side] = product(cells(k, side), matrix)
        for side in (1, 0):
            send_part(k, side).wait_recv()
            more = product(part[2 * k + side], part_matrix)
            emit(k, side, partial[side] + more)
        start_x(k)
        return 0

    cell = lax.broadcasted_iota(jnp.int32, (32, 128), 0)
    has_below = filled((gy > 0).astype(F32), (32, 128)) > 0.5
    high_y = 1.0 - share(cell.astype(F32))

    def z_copy(k):
        t = target(k)
        return pltpu.make_async_remote_copy(
            src_ref=folded.at[t],
            dst_ref=slots.at[zc],
            send_sem=z_send.at[t],
            recv_sem=z_recv.at[zc],
            device_id=(2 * t + xl, gy, gz),
            device_id_type=MESH,
        )

    def forward(k, dst, place):
        t = target(k)
        low, *high = x_copies(k)
        low.wait_recv()

        @pl.when(gy > 0)
        def _():
            for copy in high:
                copy.wait_recv()

        for u in range(4):
            same = own[t, u]
            more = high_y * (decode(got_up_same[t, u], dither[u]) - same)
            same += jnp.where(has_below, more, 0.0)
            cross = decode(got_low_cross[t, u], dither[u])
            more = high_y * (decode(got_up_cross[t, u], dither[u]) - cross)
            cross += jnp.where(has_below, more, 0.0)
            dst[place, 4 * xl + u] = encode(same, dither[4 + u])
            dst[place, 4 * xo + u] = encode(cross, dither[4 + u])

    def pass_on(k, _):
        @pl.when((half == 0) & (k == 3))
        def _():
            pl.semaphore_wait(far_sem, 4)

        forward(k, folded, target(k))
        z_copy(k).start()
        return 0

    def step(k, _):
        @pl.when(gz == 0)
        def _():
            fold_first(k, 0)

        @pl.when(gz == 1)
        def _():
            fold_second(k, 0)

        @pl.when(k >= 3)
        def _():
            pass_on(k - 3, 0)

        return 0

    lax.fori_loop(0, 8, step, 0)
    lax.fori_loop(5, 7, pass_on, 0)
    forward(jnp.int32(7), slots, zc)

    def await_slot(s):
        @pl.when(zc != s)
        def _():
            pltpu.make_async_remote_copy(
                src_ref=folded.at[0],
                dst_ref=slots.at[s],
                send_sem=z_send.at[0],
                recv_sem=z_recv.at[s],
                device_id=partner,
                device_id_type=MESH,
            ).wait_recv()

    has_before = (gx >= 1).astype(F32)

    def softmax(s, _):
        await_slot(s)
        await_slot(s + 4)
        for i in range(8):
            x = 8 * s + i
            high_x = (1.0 - share(filled(x.astype(F32), (1, 128)))) * has_before
            near = decode(slots[s, i], dither[4 + i % 4])
            far = decode(slots[s + 4, i], dither[4 + i % 4])
            d = near + high_x * (far - near)
            top = jnp.maximum(jnp.maximum(d, pltpu.roll(d, 64, 1)), 0.0)
            e = jnp.exp(d - top)
            p = e / (e + pltpu.roll(e, 64, 1) + jnp.exp(-top))
            prob[x] = p
            block[x] = p.astype(WIRE)
            rows[0, pl.ds(x, 1)] = p[0:1]
            rows[1, pl.ds(x, 1)] = p[31:32]
        return 0

    lax.fori_loop(0, 4, softmax, 0)
    sent_rows[...] = rows[0:2].astype(WIRE)
    for i in range(2):
        for j in range(2):
            corners[2 * i + j] = rows[j, 31 * i : 31 * i + 1]

    halos = []

    def exchange(src, dst, i, j, to):
        n = len(halos)
        copy = pltpu.make_async_remote_copy(
            src_ref=src,
            dst_ref=dst,
            send_sem=h_send.at[n],
            recv_sem=h_recv.at[n],
            device_id=(gx_by[i], gy_by[j], to),
            device_id_type=MESH,
        )
        out, back = there_x[i] & there_y[j], there_x[-i] & there_y[-j]
        halos.append((copy, out, back))
        pl.when(out)(copy.start)

    for other in range(2):
        to = 1 - gz if other else gz
        for i in range(2):
            for j in range(2):
                exchange(
                    corners.at[2 * i + j],
                    got_corners.at[other, 2 * (1 - i) + 1 - j],
                    2 * i - 1,
                    2 * j - 1,
                    to,
                )
    for other in range(2):
        to = 1 - gz if other else gz
        for i in range(2):
            exchange(sent_rows.at[i], got_rows.at[other, 1 - i], 0, 2 * i - 1, to)
        for i in range(2):
            exchange(block.at[31 * i], got_planes.at[other, 1 - i], 2 * i - 1, 0, to)
    exchange(block, got_block, 0, 0, 1 - gz)

    def sum_z(p, q):
        p, q = p.astype(F32), q.astype(F32)
        at = lax.rem(lax.broadcasted_iota(jnp.int32, p.shape, 1), 64)
        upper = filled(gz.astype(F32), p.shape)
        edge = pltpu.roll(q, 63 + 2 * gz, 1)
        before = jnp.where(at == 0, edge * upper, pltpu.roll(p, 1, 1))
        after = jnp.where(at == 63, edge * (1.0 - upper), pltpu.roll(p, 127, 1))
        return before + p + after

    halos[-1][0].wait_recv()

    def sum_block(s, _):
        for i in range(4):
            sums[4 * s + i + 1] = sum_z(prob[4 * s + i], got_block[4 * s + i])
        return 0

    lax.fori_loop(0, 8, sum_block, 0)
    for copy, _, back in halos[:-1]:
        pl.when(back)(copy.wait_recv)

    def inside(value, condition):
        return jnp.where(filled(condition.astype(F32), value.shape) > 0.5, value, 0.0)

    for i in range(2):
        here = there_x[2 * i - 1]
        sums[33 * i] = inside(sum_z(got_planes[0, i], got_planes[1, i]), here)
    for j in range(2):
        here = there_y[2 * j - 1]
        side_sums[j, 1:33] = inside(sum_z(got_rows[0, j], got_rows[1, j]), here)
        for i in range(2):
            n = 2 * i + j
            corner = sum_z(
                jnp.broadcast_to(got_corners[0, n], (8, 128)),
                jnp.broadcast_to(got_corners[1, n], (8, 128)),
            )
            here = there_x[2 * i - 1] & there_y[2 * j - 1]
            side_sums[j, 33 * i : 33 * i + 1] = inside(corner, here)[0:1]

    @pl.when(gz == 0)
    def _():
        def finish(k, _):
            send_part(k, 0).wait_send()
            send_part(k, 1).wait_send()
            return 0

        lax.fori_loop(0, 8, finish, 0)

    def finish(k, _):
        low, *high = x_copies(k)
        low.wait_send()

        @pl.when(gy < 7)
        def _():
            for copy in high:
                copy.wait_send()

        return 0

    lax.fori_loop(0, 8, finish, 0)

    def finish_z(k, _):
        z_copy(k).wait_send()
        return 0

    lax.fori_loop(0, 7, finish_z, 0)
    for copy, out, _ in halos:
        pl.when(out)(copy.wait_send)


def box(sums, side_sums, smooth, conf, sides, smooth_block, conf_block, sems):
    gx, gy, gz = lax.axis_index("gx"), lax.axis_index("gy"), lax.axis_index("gz")
    lane = lax.rem(lax.broadcasted_iota(jnp.int32, (32, 128), 1), 64)
    cell = lax.broadcasted_iota(jnp.int32, (32, 128), 0)

    def cut(place, at, there):
        return jnp.where(place == at, filled(there.astype(F32), (32, 128)), 0.0)

    count_y = 3.0 - cut(cell, 0, gy == 0) - cut(cell, 31, gy == 7)
    count_z = 3.0 - cut(lane, 0, gz == 0) - cut(lane, 63, gz == 1)
    inverse = 1.0 / (count_y * count_z)
    for j in range(2):
        sides[j] = side_sums[j, 0:32] + side_sums[j, 1:33] + side_sums[j, 2:34]

    def plane(x):
        s = sums[x] + sums[x + 1] + sums[x + 2]
        low = jnp.broadcast_to(sides[0, pl.ds(x, 1)], (32, 128))
        high = jnp.broadcast_to(sides[1, pl.ds(x, 1)], (32, 128))
        before = jnp.where(cell == 0, low, pltpu.roll(s, 1, 0))
        after = jnp.where(cell == 31, high, pltpu.roll(s, 31, 0))
        end = ((gx == 0) & (x == 0)) | ((gx == 15) & (x == 31))
        count_x = 3.0 - filled(end.astype(F32), (32, 128))
        s1 = (before + s + after) * (inverse / count_x)
        s2 = pltpu.roll(s1, 64, 1)
        s0 = 1.0 - s1 - s2
        smooth_block[0, x] = s0[:, :64]
        smooth_block[1, x] = s1[:, :64]
        smooth_block[2, x] = s2[:, :64]
        conf_block[x] = jnp.maximum(jnp.maximum(s0, s1), s2)[:, :64]

    def copies(n):
        part = pl.ds(n * (32 // PARTS), 32 // PARTS)
        return (
            pltpu.make_async_copy(smooth_block.at[:, part], smooth.at[:, part], sems.at[0, n]),
            pltpu.make_async_copy(conf_block.at[part], conf.at[part], sems.at[1, n]),
        )

    for n in range(PARTS):

        def some(x, _):
            for i in range(4):
                plane(4 * x + i)
            return 0

        lax.fori_loop(n * (8 // PARTS), (n + 1) * (8 // PARTS), some, 0)
        for copy in copies(n):
            copy.start()
    for n in range(PARTS):
        for copy in copies(n):
            copy.wait()


def per_device(patches):
    vmem = pltpu.VMEM
    dma = pltpu.SemaphoreType.DMA
    in_hbm = pl.BlockSpec(memory_space=pltpu.HBM)
    in_vmem = pl.BlockSpec(memory_space=pltpu.VMEM)
    sums, side_sums = pl.pallas_call(
        kernel,
        name="stitch",
        out_shape=(
            jax.ShapeDtypeStruct((34, 32, 128), F32),
            jax.ShapeDtypeStruct((2, 48, 128), F32),
        ),
        in_specs=[in_hbm],
        out_specs=(in_vmem, in_vmem),
        scratch_shapes=[
            vmem((16, 3, 4, 64, 128), jnp.bfloat16),
            vmem((16, 256, 128), WIRE),
            vmem((16, 256, 128), WIRE),
            vmem((2, 256, 128), F32),
            vmem((384, 256), WIRE),
            vmem((128, 256), WIRE),
            vmem((384, 128), WIRE),
            vmem((8, 4, 32, 128), F32),
            *[vmem((8, 4, 32, 128), WIRE)] * 6,
            vmem((8, 8, 32, 128), WIRE),
            vmem((8, 8, 32, 128), WIRE),
            vmem((8, 32, 128), F32),
            vmem((32, 32, 128), F32),
            vmem((32, 32, 128), WIRE),
            vmem((32, 32, 128), WIRE),
            vmem((3, 32, 128), F32),
            vmem((2, 32, 128), WIRE),
            vmem((16, 1, 128), F32),
            vmem((2, 2, 32, 128), WIRE),
            vmem((2, 2, 32, 128), WIRE),
            vmem((4, 4, 1, 128), F32),
            pltpu.SemaphoreType.REGULAR,
            dma((16,)),
            dma((2, 16)),
            dma((3, 8)),
            dma((3, 8)),
            dma((8,)),
            dma((8,)),
            dma((17,)),
            dma((17,)),
        ],
        compiler_params=pltpu.CompilerParams(
            collective_id=0, has_side_effects=True, vmem_limit_bytes=52 << 20
        ),
    )(patches)
    return pl.pallas_call(
        box,
        name="box",
        out_shape=(
            jax.ShapeDtypeStruct((3, 32, 32, 64), F32),
            jax.ShapeDtypeStruct((32, 32, 64), F32),
        ),
        in_specs=[in_vmem, in_vmem],
        out_specs=(in_hbm, in_hbm),
        scratch_shapes=[
            vmem((3, 32, 128), F32),
            vmem((3, 32, 32, 64), F32),
            vmem((32, 32, 64), F32),
            dma((2, PARTS)),
        ],
        compiler_params=pltpu.CompilerParams(vmem_limit_bytes=20 << 20),
    )(sums, side_sums)


def solution(mesh):
    in_specs = (P(None, "gy", None, "gx", None, "gz"),)
    out_specs = (P(None, "gx", "gy", "gz"), P("gx", "gy", "gz"))
    return jax.shard_map(
        per_device, mesh=mesh, in_specs=in_specs, out_specs=out_specs, check_vma=False
    )
```
